32 devices in a mesh: grp: 4 (over x, core), dev: 8 (over z, y).
Axes of the slice: x: 2, y: 2, z: 4, core: 2. Of those that a mesh axis runs over, the one named last changes fastest.
Arguments:
- fields: float32 [24, 64, 128, 128], P(None, ('grp', 'dev')), may hold values from -6 to 6
- mix_matrix: float32 [24, 24], replicated, may hold values from -1.25 to 1.25
- laplace_matrix: float32 [24, 24], replicated, may hold values from -0.21875 to 0.21875
Outputs:
- rhs: float32 [24, 64, 128, 128], P(None, ('grp', 'dev'))
- weyl: float32 [2, 64, 128, 128], P(None, 'grp', 'dev')
The draws below stay inside these ranges and needn't reach their ends.
All inputs are finite; a program needn't handle non-finite values.
Results may differ from the reference program's by a relative error of at most 0.0003.
Values sent between devices are 32-bit elements; how exact they have to be, the bound alone decides.
A program may use at most 192 MiB of HBM per device.

```python
import jax
import jax.numpy as jnp
from jax import lax

FIELDS = 24
CZ = 2
NY = 128
NX = 128
NZ = 64


def block_scale(key, dims, split, smallest, top_value):
    level = 1.0
    for position, blocks in split:
        draws = jax.random.uniform(jax.random.fold_in(jax.random.fold_in(key, 6), position), (blocks,), jnp.float32, smallest / len(split), top_value / len(split))
        level = level * jnp.repeat(jnp.exp(draws), dims[position] // blocks).reshape((-1,) + (1,) * (len(dims) - 1 - position))
    return level


def normal_values(stream_key, shape, scale, reach, split=(), kind=jnp.bfloat16):
    values = scale * jax.random.normal(stream_key, shape, jnp.float32)
    if split:
        values = values * block_scale(stream_key, shape, split, -0.22, 0.18)
    return jnp.clip(values, -reach, reach).astype(kind)


def setup_inputs(seed: int = 0) -> dict:
    keys = jax.random.split(jax.random.key(seed), 4)
    fields = normal_values(keys[0], (FIELDS, NZ, NY, NX), 1.0, 6.0, ((1, 32),), jnp.float32)
    mix_matrix = normal_values(keys[1], (FIELDS, FIELDS), FIELDS ** -0.5, 1.25, (), jnp.float32)
    laplace_matrix = normal_values(keys[2], (FIELDS, FIELDS), (FIELDS * 30) ** -0.5, 0.21875, (), jnp.float32)
    return {"fields": fields, "mix_matrix": mix_matrix, "laplace_matrix": laplace_matrix}


def pad_periodic(field, dimension):
    length = field.shape[dimension]
    before = lax.slice_in_dim(field, length - 2, length, axis=dimension)
    after = lax.slice_in_dim(field, 0, 2, axis=dimension)
    return jnp.concatenate([before, field, after], axis=dimension)

def interior(padded, keep):
    result = padded
    for dimension in (1, 2, 3):
        if dimension != keep:
            result = lax.slice_in_dim(result, 2, result.shape[dimension] - 2, axis=dimension)
    return result

def stencil_values(padded, dimension):
    centre = interior(padded, dimension)
    length = centre.shape[dimension] - 4
    return [lax.slice_in_dim(centre, offset, offset + length, axis=dimension) for offset in range(5)]

def first_diff(padded, dimension):
    values = stencil_values(padded, dimension)
    return (values[0] - 8.0 * values[1] + 8.0 * values[3] - values[4]) / 12.0

def second_diff(padded, dimension):
    values = stencil_values(padded, dimension)
    return (-values[0] + 16.0 * values[1] - 30.0 * values[2] + 16.0 * values[3] - values[4]) / 12.0

def laplacian(padded):
    return second_diff(padded, 1) + second_diff(padded, 2) + second_diff(padded, 3)

def evolution(padded, mix_matrix, laplace_matrix):
    centre = interior(padded, 0)
    laplace = laplacian(padded)
    result = jnp.einsum('fg,gzyx->fzyx', mix_matrix, centre, precision=lax.Precision.HIGHEST)
    result = result + jnp.einsum('fg,gzyx->fzyx', laplace_matrix, laplace, precision=lax.Precision.HIGHEST)
    for dimension in (1, 2, 3):
        result = result + centre[11 + dimension][None] * first_diff(padded, dimension)
    return result

def contract(tensor, left, right):
    total = 0.0
    for first in range(3):
        for second in range(3):
            total = total + tensor[first][second] * left[first] * right[second]
    return total

def weyl_scalar(padded, zpos, ypos, xpos):
    table = ((0, 1, 2), (1, 3, 4), (2, 4, 5))
    metric = padded[0:6]
    curv_padded = padded[6:12]
    lap_metric = laplacian(metric)
    curvature = interior(curv_padded, 0)
    gradient = [first_diff(curv_padded, 3 - index) for index in range(3)]
    trace = curvature[0] + curvature[3] + curvature[5]
    electric = []
    curl = []
    for first in range(3):
        erow = []
        crow = []
        for second in range(3):
            value = -0.5 * lap_metric[table[first][second]] - trace * curvature[table[first][second]]
            for middle in range(3):
                value = value + curvature[table[first][middle]] * curvature[table[middle][second]]
            erow.append(value)
            next_one = (first + 1) % 3
            next_two = (first + 2) % 3
            crow.append(gradient[next_one][table[next_two][second]] - gradient[next_two][table[next_one][second]])
        electric.append(erow)
        curl.append(crow)
    magnetic = [[0.5 * (curl[first][second] + curl[second][first]) for second in range(3)] for first in range(3)]
    along_x = xpos[None, None, :]
    along_y = ypos[None, :, None]
    along_z = zpos[:, None, None]
    cylinder = jnp.sqrt(along_x * along_x + along_y * along_y)
    radius = jnp.sqrt(cylinder * cylinder + along_z * along_z)
    theta_vec = (along_z * along_x / (radius * cylinder), along_z * along_y / (radius * cylinder), -cylinder / radius)
    phi_vec = (-along_y / cylinder, along_x / cylinder, 0.0)
    real_part = 0.5 * (contract(electric, theta_vec, theta_vec) - contract(electric, phi_vec, phi_vec)) - contract(magnetic, theta_vec, phi_vec)
    imag_part = -contract(electric, theta_vec, phi_vec) - 0.5 * (contract(magnetic, theta_vec, theta_vec) - contract(magnetic, phi_vec, phi_vec))
    shape = curvature.shape[1:]
    return jnp.stack([jnp.broadcast_to(real_part, shape), jnp.broadcast_to(imag_part, shape)])

def centred(index, count):
    return index.astype(jnp.float32) + 0.5 - 0.5 * count

def reference(fields, mix_matrix, laplace_matrix):
    rows = fields.shape[2]
    width = fields.shape[3]
    padded = pad_periodic(pad_periodic(pad_periodic(fields, 1), 2), 3)
    ypos = centred(jnp.arange(rows, dtype=jnp.int32), rows)
    xpos = centred(jnp.arange(width, dtype=jnp.int32), width)

    def block(index):
        start = (index * CZ).astype(jnp.int32)
        window = lax.dynamic_slice_in_dim(padded, start, CZ + 4, axis=1)
        zpos = centred(start + jnp.arange(CZ, dtype=jnp.int32), NZ)
        return (evolution(window, mix_matrix, laplace_matrix), weyl_scalar(window[0:12], zpos, ypos, xpos))
    rhs_blocks, weyl_blocks = lax.map(block, jnp.arange(NZ // CZ, dtype=jnp.int32))
    rhs = jnp.transpose(rhs_blocks, (1, 0, 2, 3, 4)).reshape(FIELDS, NZ, rows, width)
    weyl = jnp.transpose(weyl_blocks, (1, 0, 2, 3, 4)).reshape(2, NZ, rows, width)
    return (rhs, weyl)
```

```python
import functools

import jax
import jax.numpy as jnp
from jax import lax
from jax.experimental import pallas as pl
from jax.experimental.pallas import tpu as pltpu
from jax.sharding import PartitionSpec as P

AHEAD = 6
LAG = 4
WEYL_STEPS = 4
TABLE = ((0, 1, 2), (1, 3, 4), (2, 4, 5))
PAIRS = ((0, 0), (0, 1), (0, 2), (1, 1), (1, 2), (2, 2))


def contract(tensor, left, right):
    total = None
    for first in range(3):
        for second in range(3):
            if left[first] is None or right[second] is None:
                continue
            term = tensor[TABLE[first][second]] * (left[first] * right[second])
            total = term if total is None else total + term
    return total


def weyl_pair(curv, lap, grad, along_x, along_y, along_z):
    trace = curv[0] + curv[3] + curv[5]
    electric = []
    for first, second in PAIRS:
        spot = TABLE[first][second]
        value = -0.5 * lap[spot] - trace * curv[spot]
        for middle in range(3):
            value = value + curv[TABLE[first][middle]] * curv[TABLE[middle][second]]
        electric.append(value)

    def curl(first, second):
        one = (first + 1) % 3
        two = (first + 2) % 3
        return grad[one][TABLE[two][second]] - grad[two][TABLE[one][second]]

    magnetic = [0.5 * (curl(first, second) + curl(second, first)) for first, second in PAIRS]
    square = along_x * along_x + along_y * along_y
    cylinder = jnp.sqrt(square)
    radius = jnp.sqrt(square + along_z * along_z)
    over_cyl = 1.0 / cylinder
    over_rad = 1.0 / radius
    slope = along_z * over_rad * over_cyl
    theta = (slope * along_x, slope * along_y, -cylinder * over_rad)
    phi = (-along_y * over_cyl, along_x * over_cyl, None)
    real = 0.5 * (contract(electric, theta, theta) - contract(electric, phi, phi)) - contract(
        magnetic, theta, phi
    )
    imag = -contract(electric, theta, phi) - 0.5 * (
        contract(magnetic, theta, theta) - contract(magnetic, phi, phi)
    )
    return real, imag


def kernel(
    groups,
    members,
    fields_ref,
    mix_hbm,
    lap_hbm,
    rhs_ref,
    weyl_ref,
    own,
    halo,
    lapbuf,
    laph,
    gradk,
    wtmp,
    wloc,
    wrecv,
    mix_ref,
    lap_ref,
    own_sem,
    mat_sem,
    send_p,
    recv_p,
    send_r,
    recv_r,
    send_e,
    send_w,
    recv_w,
    chain_sem,
    wrap_sem,
    ready_sem,
):
    count, depth, rows, width = own.shape
    slabs = groups * members
    grp = lax.axis_index("grp")
    dev = lax.axis_index("dev")
    slab = grp * members + dev
    side = lax.rem(slab, 2)
    step = 2 - 4 * side
    partner = slab + 1 - 2 * side
    follow = lax.rem(slab + slabs + step, slabs)
    far = lax.rem(slab + slabs - 1 + 2 * side, slabs)
    per = rows // members
    first = jnp.where(side == 0, dev < 2, dev >= members - 2)
    last = jnp.where(side == 0, dev >= members - 2, dev < 2)
    ahead_grp = lax.rem(grp + groups + 1 - 2 * side, groups)
    behind_grp = lax.rem(grp + groups - 1 + 2 * side, groups)
    middle = (dev == 0) | (dev == members // 2 - 1) | (dev == members // 2) | (dev == members - 1)

    def place(index):
        return (index // members, lax.rem(index, members))

    def signal(semaphore, target):
        pl.semaphore_signal(
            semaphore, inc=1, device_id=target, device_id_type=pl.DeviceIdType.MESH
        )

    barrier = pltpu.get_barrier_semaphore()
    signal(barrier, place(partner))

    @pl.when(jnp.logical_not(last))
    def _():
        signal(barrier, (grp, dev + step))

    @pl.when(jnp.logical_not(first))
    def _():
        signal(barrier, (grp, dev - step))

    @pl.when(last)
    def _():
        signal(barrier, (ahead_grp, dev))

    load = pltpu.make_async_copy(fields_ref, own, own_sem)
    small = (
        pltpu.make_async_copy(mix_hbm, mix_ref, mat_sem.at[0]),
        pltpu.make_async_copy(lap_hbm, lap_ref, mat_sem.at[1]),
    )

    def remote(source, target, send, recv, device):
        return pltpu.make_async_remote_copy(
            src_ref=source,
            dst_ref=target,
            send_sem=send,
            recv_sem=recv,
            device_id=device,
            device_id_type=pl.DeviceIdType.MESH,
        )

    def peer(offset):
        return lax.rem(dev + offset, members)

    chunks = count * depth
    final = count - 1
    ahead = min(AHEAD, chunks)
    ring = 2 * ahead

    def exchange(i, slot):
        g, p = i // depth, lax.rem(i, depth)
        return remote(
            fields_ref.at[g, p], halo.at[slot, g, p], send_p, recv_p.at[lax.rem(i, ring)], place(partner)
        )

    def relay(g, p, slot, send):
        recv = recv_r.at[g] if p is None or not isinstance(g, int) else recv_r.at[g + p]
        return remote(halo.at[1 - side, g, p], halo.at[slot, g, p], send, recv, place(follow))

    direct = remote(
        fields_ref.at[final, depth - 1],
        halo.at[1 - side, final, depth - 1],
        send_e.at[2],
        recv_r.at[final + 1],
        place(far),
    )

    def spread(target, source):
        return remote(wloc.at[target], wrecv.at[source], send_w, recv_w, (grp, target))

    pl.semaphore_wait(barrier, jnp.where(first, 2, 3))

    @pl.loop(0, ahead)
    def _(i):
        exchange(i, side).start()

    load.start()
    for copy in small:
        copy.start()

    @pl.when(jnp.logical_not(last))
    def _():
        signal(ready_sem, place(partner))

    @pl.when(first)
    def _():
        signal(chain_sem, (grp, dev + step))

    @pl.when(jnp.logical_not(first))
    def _():
        pl.semaphore_wait(chain_sem, 1)

        @pl.when(last)
        def _():
            signal(wrap_sem, (behind_grp, dev))

        @pl.when(jnp.logical_not(last))
        def _():
            signal(chain_sem, (grp, dev + step))

    @pl.when(last)
    def _():
        pl.semaphore_wait(wrap_sem, 1)
        signal(ready_sem, place(partner))

    pl.semaphore_wait(ready_sem, 1)

    @pl.when(middle)
    def _():
        direct.start()

    def advance(i):
        exchange(i, 1 - side).wait_recv()
        g, p = i // depth, lax.rem(i, depth)

        @pl.when(g < final)
        def _():
            relay(g, p, side, send_r).start()

        @pl.when(i == chunks - 2)
        def _():
            relay(final, 0, side, send_e.at[0]).start()

        @pl.when((i == chunks - 1) & middle)
        def _():
            relay(final, 1, side, send_e.at[1]).start()

        @pl.when(i + ahead < chunks)
        def _():
            exchange(i + ahead, side).start()

    @pl.loop(0, LAG * depth)
    def _(i):
        advance(i)

    rhs_ref[...] = jnp.zeros_like(rhs_ref)
    load.wait()
    for copy in small:
        copy.wait()

    def relayed(g):
        @pl.when(g < final)
        def _():
            remote(halo.at[side, g], halo.at[side, g], send_r, recv_r.at[g], place(follow)).wait_recv()

        @pl.when(g == final)
        def _():
            relay(final, 0, side, send_e.at[0]).wait_recv()
            relay(final, 1, side, send_e.at[1]).wait_recv()

    def weyl_local(part):
        tiles = rows // 8
        share = depth * tiles // WEYL_STEPS

        @pl.loop(0, share)
        def _(u):
            t = part * share + u
            p = t // tiles
            start = pl.multiple_of(lax.rem(t, tiles) * 8, 8)
            strip = pl.ds(start, 8)
            curv = [own[6 + n, p, strip, :] for n in range(6)]
            lap = [laph[n, p, strip, :] for n in range(6)]
            grad = [[gradk[n, a, p, strip, :] for n in range(6)] for a in range(3)]
            lane = lax.broadcasted_iota(jnp.int32, (8, width), 1)
            row = lax.broadcasted_iota(jnp.int32, (8, width), 0) + start
            layer = jnp.full((8, width), slab * depth + p, jnp.int32)
            along_x = lane.astype(jnp.float32) + (0.5 - 0.5 * width)
            along_y = row.astype(jnp.float32) + (0.5 - 0.5 * rows)
            along_z = layer.astype(jnp.float32) + (0.5 - 0.5 * depth * slabs)
            real, imag = weyl_pair(curv, lap, grad, along_x, along_y, along_z)
            wtmp[0, p, strip, :] = real
            wtmp[1, p, strip, :] = imag

    def process(g, p):
        f = own[g, p]
        planes = [halo[0, g, 0], halo[0, g, 1], own[g, 0], own[g, 1], halo[1, g, 0], halo[1, g, 1]]
        zm2, zm1, _, zp1, zp2 = planes[p : p + 5]
        ym1, ym2 = pltpu.roll(f, 1, 0), pltpu.roll(f, 2, 0)
        yp1, yp2 = pltpu.roll(f, rows - 1, 0), pltpu.roll(f, rows - 2, 0)
        xm1, xm2 = pltpu.roll(f, 1, 1), pltpu.roll(f, 2, 1)
        xp1, xp2 = pltpu.roll(f, width - 1, 1), pltpu.roll(f, width - 2, 1)
        near = ((zm1 + zp1) + (ym1 + yp1)) + (xm1 + xp1)
        far_sum = ((zm2 + zp2) + (ym2 + yp2)) + (xm2 + xp2)
        lap = (16.0 * near - far_sum - 90.0 * f) * (1.0 / 12.0)
        lapbuf[p] = lap
        gz = (8.0 * (zp1 - zm1) - (zp2 - zm2)) * (1.0 / 12.0)
        gy = (8.0 * (yp1 - ym1) - (yp2 - ym2)) * (1.0 / 12.0)
        gx = (8.0 * (xp1 - xm1) - (xp2 - xm2)) * (1.0 / 12.0)
        rhs_ref[g, p] += own[12, p] * gz + own[13, p] * gy + own[14, p] * gx

        @pl.when(g < 6)
        def _():
            laph[g, p] = lap

        @pl.when(jnp.logical_and(g >= 6, g < 12))
        def _():
            gradk[g - 6, 0, p] = gx
            gradk[g - 6, 1, p] = gy
            gradk[g - 6, 2, p] = gz

        size = 32

        @pl.loop(0, rows // size)
        def _(t):
            strip = pl.ds(pl.multiple_of(t * size, size), size)
            f = own[g, p, strip, :]
            lap = lapbuf[p, strip, :]
            for c in range(count):
                rhs_ref[c, p, strip, :] += mix_ref[c, g] * f + lap_ref[c, g] * lap

    @pl.loop(0, count)
    def _(g):
        more = g + LAG < count

        @pl.when(more)
        def _():
            advance((g + LAG) * depth)

        relayed(g)
        process(g, 0)

        @pl.when(more)
        def _():
            advance((g + LAG) * depth + 1)

        process(g, 1)

        @pl.when(jnp.logical_and(g >= 11, g < 11 + WEYL_STEPS))
        def _():
            weyl_local(g - 11)

        @pl.when(g == 11 + WEYL_STEPS)
        def _():
            for m in range(members):
                wloc[m] = wtmp[:, :, m * per : (m + 1) * per, :]

        @pl.when(g == 12 + WEYL_STEPS)
        def _():
            for offset in range(1, members):
                spread(peer(offset), dev).start()

    def put(source, block):
        for comp in range(2):
            for p in range(depth):
                weyl_ref[comp, source * depth + p] = block[comp, p]

    others = pl.ds(0, members - 1)
    remote(wrecv.at[others], wrecv.at[others], send_w, recv_w, (grp, dev)).wait_recv()
    put(dev, wloc.at[dev])
    for offset in range(1, members):
        source = peer(offset)
        put(source, wrecv.at[source])
    remote(wloc.at[others], wloc.at[others], send_w, recv_w, (grp, dev)).wait_send()
    remote(fields_ref, halo.at[0], send_p, recv_p.at[0], place(partner)).wait_send()
    early = pl.ds(0, final)
    remote(halo.at[0, early], halo.at[0, early], send_r, recv_r.at[0], place(follow)).wait_send()
    relay(final, 0, side, send_e.at[0]).wait_send()

    @pl.when(middle)
    def _():
        relay(final, 1, side, send_e.at[1]).wait_send()
        direct.wait_send()


def per_device(groups, members, fields, mix_matrix, laplace_matrix):
    count, depth, rows, width = fields.shape
    assert depth == 2 and members % 4 == 0
    plane = (rows, width)
    per = rows // members
    vmem = functools.partial(pltpu.VMEM, dtype=jnp.float32)
    dma = pltpu.SemaphoreType.DMA
    return pl.pallas_call(
        functools.partial(kernel, groups, members),
        out_shape=(
            jax.ShapeDtypeStruct(fields.shape, jnp.float32),
            jax.ShapeDtypeStruct((2, depth * members, per, width), jnp.float32),
        ),
        in_specs=[
            pl.BlockSpec(memory_space=pltpu.HBM),
            pl.BlockSpec(memory_space=pltpu.HBM),
            pl.BlockSpec(memory_space=pltpu.HBM),
        ],
        out_specs=(
            pl.BlockSpec(memory_space=pltpu.VMEM),
            pl.BlockSpec(memory_space=pltpu.VMEM),
        ),
        scratch_shapes=[
            vmem((count, depth) + plane),
            vmem((2, count, depth) + plane),
            vmem((depth,) + plane),
            vmem((6, depth) + plane),
            vmem((6, 3, depth) + plane),
            vmem((2, depth) + plane),
            vmem((members, 2, depth, per, width)),
            vmem((members, 2, depth, per, width)),
            pltpu.SMEM((count, count), jnp.float32),
            pltpu.SMEM((count, count), jnp.float32),
            dma,
            dma((2,)),
            dma,
            dma((2 * min(AHEAD, count * depth),)),
            dma,
            dma((count + 1,)),
            dma((3,)),
            dma,
            dma,
            pltpu.SemaphoreType.REGULAR,
            pltpu.SemaphoreType.REGULAR,
            pltpu.SemaphoreType.REGULAR,
        ],
        compiler_params=pltpu.CompilerParams(
            collective_id=0, has_side_effects=True, vmem_limit_bytes=48 * 1024 * 1024
        ),
        name="evolve",
    )(
        fields,
        pltpu.with_memory_space_constraint(mix_matrix, pltpu.HBM),
        pltpu.with_memory_space_constraint(laplace_matrix, pltpu.HBM),
    )


def solution(mesh):
    groups, members = mesh.shape["grp"], mesh.shape["dev"]
    return jax.shard_map(
        functools.partial(per_device, groups, members),
        mesh=mesh,
        in_specs=(P(None, ("grp", "dev"), None, None), P(), P()),
        out_specs=(P(None, ("grp", "dev"), None, None), P(None, "grp", "dev", None)),
        check_vma=False,
    )
```

```python
import functools

import jax
import jax.numpy as jnp
from jax import lax
from jax.experimental import pallas as pl
from jax.experimental.pallas import tpu as pltpu
from jax.sharding import PartitionSpec as P

AHEAD = 12
LAG = 4
WEYL_STEPS = 4
STRIP = 32
HALVES = 2
TABLE = ((0, 1, 2), (1, 3, 4), (2, 4, 5))
PAIRS = ((0, 0), (0, 1), (0, 2), (1, 1), (1, 2), (2, 2))


def contract(tensor, left, right):
    total = None
    for first in range(3):
        for second in range(3):
            if left[first] is None or right[second] is None:
                continue
            term = tensor[TABLE[first][second]] * (left[first] * right[second])
            total = term if total is None else total + term
    return total


def weyl_pair(curv, lap, grad, along_x, along_y, along_z):
    trace = curv[0] + curv[3] + curv[5]
    electric = []
    for first, second in PAIRS:
        spot = TABLE[first][second]
        value = -0.5 * lap[spot] - trace * curv[spot]
        for middle in range(3):
            value = value + curv[TABLE[first][middle]] * curv[TABLE[middle][second]]
        electric.append(value)

    def curl(first, second):
        one = (first + 1) % 3
        two = (first + 2) % 3
        return grad[one][TABLE[two][second]] - grad[two][TABLE[one][second]]

    magnetic = [0.5 * (curl(first, second) + curl(second, first)) for first, second in PAIRS]
    square = along_x * along_x + along_y * along_y
    cylinder = jnp.sqrt(square)
    radius = jnp.sqrt(square + along_z * along_z)
    over_cyl = 1.0 / cylinder
    over_rad = 1.0 / radius
    slope = along_z * over_rad * over_cyl
    theta = (slope * along_x, slope * along_y, -cylinder * over_rad)
    phi = (-along_y * over_cyl, along_x * over_cyl, None)
    real = 0.5 * (contract(electric, theta, theta) - contract(electric, phi, phi)) - contract(
        magnetic, theta, phi
    )
    imag = -contract(electric, theta, phi) - 0.5 * (
        contract(magnetic, theta, theta) - contract(magnetic, phi, phi)
    )
    return real, imag


def kernel(
    groups,
    members,
    fields_ref,
    mix_hbm,
    lap_hbm,
    rhs_ref,
    wrecv,
    tail_ref,
    coef_ref,
    own,
    halo,
    lapbuf,
    laph,
    gradk,
    wtmp,
    wloc,
    mix_ref,
    lap_ref,
    own_sem,
    mat_sem,
    send_p,
    recv_p,
    send_r,
    recv_r,
    send_w,
    recv_w,
    chain_sem,
    wrap_sem,
):
    count, depth, rows, width = own.shape
    slabs = groups * members
    grp = lax.axis_index("grp")
    dev = lax.axis_index("dev")
    slab = grp * members + dev
    side = lax.rem(slab, 2)
    step = 2 - 4 * side
    partner = slab + 1 - 2 * side
    follow = lax.rem(slab + slabs + step, slabs)
    per = rows // members
    first = jnp.where(side == 0, dev < 2, dev >= members - 2)
    last = jnp.where(side == 0, dev >= members - 2, dev < 2)
    second = jnp.where(side == 0, dev // 2 == 1, dev // 2 == members // 2 - 2)
    ahead_grp = lax.rem(grp + groups + 1 - 2 * side, groups)
    behind_grp = lax.rem(grp + groups - 1 + 2 * side, groups)

    def place(index):
        return (index // members, lax.rem(index, members))

    def signal(semaphore, target):
        pl.semaphore_signal(
            semaphore, inc=1, device_id=target, device_id_type=pl.DeviceIdType.MESH
        )

    barrier = pltpu.get_barrier_semaphore()
    signal(barrier, place(partner))

    @pl.when(jnp.logical_not(last))
    def _():
        signal(barrier, (grp, dev + step))

    @pl.when(jnp.logical_not(first))
    def _():
        signal(barrier, (grp, dev - step))

    @pl.when(last)
    def _():
        signal(barrier, (ahead_grp, dev))

    load = pltpu.make_async_copy(fields_ref, own, own_sem)
    small = (
        pltpu.make_async_copy(mix_hbm, mix_ref, mat_sem.at[0]),
        pltpu.make_async_copy(lap_hbm, lap_ref, mat_sem.at[1]),
    )

    def remote(source, target, send, recv, device):
        return pltpu.make_async_remote_copy(
            src_ref=source,
            dst_ref=target,
            send_sem=send,
            recv_sem=recv,
            device_id=device,
            device_id_type=pl.DeviceIdType.MESH,
        )

    def peer(offset):
        return lax.rem(dev + offset, members)

    chunks = count * depth * HALVES
    final = count - 1
    ahead = min(AHEAD, chunks)
    ring = 2 * ahead

    half = rows // HALVES

    def split(i):
        part = pl.ds(pl.multiple_of(lax.rem(i, HALVES) * half, half), half)
        return i // (HALVES * depth), lax.rem(i // HALVES, depth), part

    def exchange(i, slot):
        g, p, part = split(i)
        return remote(
            fields_ref.at[g, p, part], halo.at[slot, g, p, part], send_p, recv_p.at[lax.rem(i, ring)], place(partner)
        )

    def relay(i, slot):
        g, p, part = split(i)
        return remote(
            halo.at[1 - side, g, p, part], halo.at[slot, g, p, part], send_r, recv_r.at[g], place(follow)
        )

    def spread(target, source):
        return remote(wloc.at[target], wrecv.at[source], send_w, recv_w, (grp, target))

    pl.semaphore_wait(barrier, jnp.where(first, 2, 3))

    @pl.loop(0, ahead)
    def _(i):
        exchange(i, side).start()

    @pl.when(jnp.logical_not(first))
    def _():
        @pl.when(jnp.logical_not(second))
        def _():
            pl.semaphore_wait(chain_sem, 1)

        @pl.when(last)
        def _():
            signal(wrap_sem, (behind_grp, dev))

        @pl.when(jnp.logical_not(last))
        def _():
            signal(chain_sem, (grp, dev + step))

    load.start()
    for copy in small:
        copy.start()

    @pl.when(last)
    def _():
        pl.semaphore_wait(wrap_sem, 1)

    def advance(i):
        exchange(i, 1 - side).wait_recv()
        relay(i, side).start()

        @pl.when(i + ahead < chunks)
        def _():
            exchange(i + ahead, side).start()

    @pl.loop(0, LAG * depth * HALVES)
    def _(i):
        advance(i)

    rhs_ref[...] = jnp.zeros_like(rhs_ref)
    load.wait()
    for copy in small:
        copy.wait()
    for c in range(count):
        for which, table in enumerate((mix_ref, lap_ref)):
            coef_ref[c, which] = jnp.full((8, width), table[c, final], jnp.float32)
    for p in range(depth):
        tail_ref[0, p] = own[final, p]

    def relayed(g):
        remote(halo.at[side, g], halo.at[side, g], send_r, recv_r.at[g], place(follow)).wait_recv()

    def weyl_local(part):
        tiles = rows // 8
        share = depth * tiles // WEYL_STEPS

        @pl.loop(0, share)
        def _(u):
            t = part * share + u
            p = t // tiles
            start = pl.multiple_of(lax.rem(t, tiles) * 8, 8)
            strip = pl.ds(start, 8)
            curv = [own[6 + n, p, strip, :] for n in range(6)]
            lap = [laph[n, p, strip, :] for n in range(6)]
            grad = [[gradk[n, a, p, strip, :] for n in range(6)] for a in range(3)]
            lane = lax.broadcasted_iota(jnp.int32, (8, width), 1)
            row = lax.broadcasted_iota(jnp.int32, (8, width), 0) + start
            layer = jnp.full((8, width), slab * depth + p, jnp.int32)
            along_x = lane.astype(jnp.float32) + (0.5 - 0.5 * width)
            along_y = row.astype(jnp.float32) + (0.5 - 0.5 * rows)
            along_z = layer.astype(jnp.float32) + (0.5 - 0.5 * depth * slabs)
            real, imag = weyl_pair(curv, lap, grad, along_x, along_y, along_z)
            wtmp[0, p, strip, :] = real
            wtmp[1, p, strip, :] = imag

    def process(g, p):
        f = own[g, p]
        planes = [halo[0, g, 0], halo[0, g, 1], own[g, 0], own[g, 1], halo[1, g, 0], halo[1, g, 1]]
        zm2, zm1, _, zp1, zp2 = planes[p : p + 5]
        ym1, ym2 = pltpu.roll(f, 1, 0), pltpu.roll(f, 2, 0)
        yp1, yp2 = pltpu.roll(f, rows - 1, 0), pltpu.roll(f, rows - 2, 0)
        xm1, xm2 = pltpu.roll(f, 1, 1), pltpu.roll(f, 2, 1)
        xp1, xp2 = pltpu.roll(f, width - 1, 1), pltpu.roll(f, width - 2, 1)
        near = ((zm1 + zp1) + (ym1 + yp1)) + (xm1 + xp1)
        far_sum = ((zm2 + zp2) + (ym2 + yp2)) + (xm2 + xp2)
        lap = (16.0 * near - far_sum - 90.0 * f) * (1.0 / 12.0)
        lapbuf[p] = lap

        @pl.when(g == final)
        def _():
            tail_ref[1, p] = lap

        gz = (8.0 * (zp1 - zm1) - (zp2 - zm2)) * (1.0 / 12.0)
        gy = (8.0 * (yp1 - ym1) - (yp2 - ym2)) * (1.0 / 12.0)
        gx = (8.0 * (xp1 - xm1) - (xp2 - xm2)) * (1.0 / 12.0)
        rhs_ref[g, p] += own[12, p] * gz + own[13, p] * gy + own[14, p] * gx

        @pl.when(g < 6)
        def _():
            laph[g, p] = lap

        @pl.when(jnp.logical_and(g >= 6, g < 12))
        def _():
            gradk[g - 6, 0, p] = gx
            gradk[g - 6, 1, p] = gy
            gradk[g - 6, 2, p] = gz

        @pl.loop(0, jnp.where(g == final, 0, rows // STRIP))
        def _(t):
            strip = pl.ds(pl.multiple_of(t * STRIP, STRIP), STRIP)
            f = own[g, p, strip, :]
            lap = lapbuf[p, strip, :]
            for c in range(count):
                rhs_ref[c, p, strip, :] += mix_ref[c, g] * f + lap_ref[c, g] * lap

    @pl.loop(0, count)
    def _(g):
        more = g + LAG < count

        @pl.when(more)
        def _():
            for k in range(HALVES):
                advance((g + LAG) * depth * HALVES + k)

        relayed(g)
        process(g, 0)

        @pl.when(more)
        def _():
            for k in range(HALVES):
                advance((g + LAG) * depth * HALVES + HALVES + k)

        process(g, 1)

        @pl.when(jnp.logical_and(g >= 11, g < 11 + WEYL_STEPS))
        def _():
            weyl_local(g - 11)

        @pl.when(g == 11 + WEYL_STEPS)
        def _():
            for m in range(members):
                wloc[m] = wtmp[:, :, m * per : (m + 1) * per, :]
            wrecv[dev] = wloc[dev]

        @pl.when(g == 12 + WEYL_STEPS)
        def _():
            for offset in range(1, members):
                spread(peer(offset), dev).start()

    others = pl.ds(0, members - 1)
    remote(wrecv.at[others], wrecv.at[others], send_w, recv_w, (grp, dev)).wait_recv()
    remote(wloc.at[others], wloc.at[others], send_w, recv_w, (grp, dev)).wait_send()
    remote(own, halo.at[0], send_p, recv_p.at[0], place(partner)).wait_send()
    remote(halo.at[0], halo.at[0], send_r, recv_r.at[0], place(follow)).wait_send()


def finish(members, part_ref, wrecv, tail_ref, coef_ref, rhs_ref, weyl_ref, whole, rhs_sem, weyl_sem):
    count, depth, rows, width = part_ref.shape
    blocks = []
    for source in range(members):
        layers = pl.ds(source * depth, depth)
        blocks.append(
            pltpu.make_async_copy(wrecv.at[source], weyl_ref.at[:, layers], weyl_sem.at[source])
        )
    for block in blocks:
        block.start()

    @pl.loop(0, depth * (rows // STRIP))
    def _(t):
        p = t // (rows // STRIP)
        start = pl.multiple_of(lax.rem(t, rows // STRIP) * STRIP, STRIP)
        strip = pl.ds(start, STRIP)
        f = [tail_ref[0, p, pl.ds(start + 8 * k, 8), :] for k in range(STRIP // 8)]
        lap = [tail_ref[1, p, pl.ds(start + 8 * k, 8), :] for k in range(STRIP // 8)]
        for c in range(count):
            mix, spread = coef_ref[c, 0], coef_ref[c, 1]
            for k in range(STRIP // 8):
                part = pl.ds(start + 8 * k, 8)
                whole[c, p, part, :] = part_ref[c, p, part, :] + (mix * f[k] + spread * lap[k])
        pltpu.make_async_copy(whole.at[:, p, strip], rhs_ref.at[:, p, strip], rhs_sem).start()

    for block in blocks:
        block.wait()
    pltpu.make_async_copy(whole, rhs_ref, rhs_sem).wait()


def per_device(groups, members, fields, mix_matrix, laplace_matrix):
    count, depth, rows, width = fields.shape
    assert depth == 2 and members % 4 == 0
    plane = (rows, width)
    per = rows // members
    vmem = functools.partial(pltpu.VMEM, dtype=jnp.float32)
    dma = pltpu.SemaphoreType.DMA
    in_hbm, in_vmem = pl.BlockSpec(memory_space=pltpu.HBM), pl.BlockSpec(memory_space=pltpu.VMEM)
    share = functools.partial(jax.ShapeDtypeStruct, dtype=jnp.float32)
    pieces = pl.pallas_call(
        functools.partial(kernel, groups, members),
        out_shape=(
            share(fields.shape),
            share((members, 2, depth, per, width)),
            share((2, depth) + plane),
            share((count, 2, 8, width)),
        ),
        in_specs=[in_hbm] * 3,
        out_specs=(in_vmem,) * 4,
        scratch_shapes=[
            vmem((count, depth) + plane),
            vmem((2, count, depth) + plane),
            vmem((depth,) + plane),
            vmem((6, depth) + plane),
            vmem((6, 3, depth) + plane),
            vmem((2, depth) + plane),
            vmem((members, 2, depth, per, width)),
            pltpu.SMEM((count, count), jnp.float32),
            pltpu.SMEM((count, count), jnp.float32),
            dma,
            dma((2,)),
            dma,
            dma((2 * min(AHEAD, count * depth * HALVES),)),
            dma,
            dma((count,)),
            dma,
            dma,
            pltpu.SemaphoreType.REGULAR,
            pltpu.SemaphoreType.REGULAR,
        ],
        compiler_params=pltpu.CompilerParams(
            collective_id=0, has_side_effects=True, vmem_limit_bytes=32 * 1024 * 1024
        ),
        name="evolve",
    )(
        pltpu.with_memory_space_constraint(fields, pltpu.HBM),
        pltpu.with_memory_space_constraint(mix_matrix, pltpu.HBM),
        pltpu.with_memory_space_constraint(laplace_matrix, pltpu.HBM),
    )
    return pl.pallas_call(
        functools.partial(finish, members),
        out_shape=(share(fields.shape), share((2, depth * members, per, width))),
        in_specs=[in_vmem] * 4,
        out_specs=(in_hbm,) * 2,
        scratch_shapes=[vmem((count, depth) + plane), dma, dma((members,))],
        compiler_params=pltpu.CompilerParams(vmem_limit_bytes=8 * 1024 * 1024),
        name="finish",
    )(*pieces)


def solution(mesh):
    groups, members = mesh.shape["grp"], mesh.shape["dev"]
    return jax.shard_map(
        functools.partial(per_device, groups, members),
        mesh=mesh,
        in_specs=(P(None, ("grp", "dev"), None, None), P(), P()),
        out_specs=(P(None, ("grp", "dev"), None, None), P(None, "grp", "dev", None)),
        check_vma=False,
    )
```

```python
import functools

import jax
import jax.numpy as jnp
from jax import lax
from jax.experimental import pallas as pl
from jax.experimental.pallas import tpu as pltpu
from jax.sharding import PartitionSpec as P

AHEAD = 12
LAG = 4
WEYL_STEPS = 4
STRIP = 32
HALVES = 2
NEAR = 2
FAR = 1
LEAVE = 8
PASS = 19
TABLE = ((0, 1, 2), (1, 3, 4), (2, 4, 5))
PAIRS = ((0, 0), (0, 1), (0, 2), (1, 1), (1, 2), (2, 2))


def contract(tensor, left, right):
    total = None
    for first in range(3):
        for second in range(3):
            if left[first] is None or right[second] is None:
                continue
            term = tensor[TABLE[first][second]] * (left[first] * right[second])
            total = term if total is None else total + term
    return total


def weyl_pair(curv, lap, grad, along_x, along_y, along_z):
    trace = curv[0] + curv[3] + curv[5]
    electric = []
    for first, second in PAIRS:
        spot = TABLE[first][second]
        value = -0.5 * lap[spot] - trace * curv[spot]
        for middle in range(3):
            value = value + curv[TABLE[first][middle]] * curv[TABLE[middle][second]]
        electric.append(value)

    def curl(first, second):
        one = (first + 1) % 3
        two = (first + 2) % 3
        return grad[one][TABLE[two][second]] - grad[two][TABLE[one][second]]

    magnetic = [0.5 * (curl(first, second) + curl(second, first)) for first, second in PAIRS]
    square = along_x * along_x + along_y * along_y
    cylinder = jnp.sqrt(square)
    radius = jnp.sqrt(square + along_z * along_z)
    over_cyl = 1.0 / cylinder
    over_rad = 1.0 / radius
    slope = along_z * over_rad * over_cyl
    theta = (slope * along_x, slope * along_y, -cylinder * over_rad)
    phi = (-along_y * over_cyl, along_x * over_cyl, None)
    real = 0.5 * (contract(electric, theta, theta) - contract(electric, phi, phi)) - contract(
        magnetic, theta, phi
    )
    imag = -contract(electric, theta, phi) - 0.5 * (
        contract(magnetic, theta, theta) - contract(magnetic, phi, phi)
    )
    return real, imag


def kernel(
    groups,
    members,
    fields_ref,
    mix_hbm,
    lap_hbm,
    rhs_ref,
    wrecv,
    tail_ref,
    coef_ref,
    own,
    halo,
    lapbuf,
    laph,
    gradk,
    wtmp,
    wloc,
    passing,
    mix_ref,
    lap_ref,
    own_sem,
    mat_sem,
    send_p,
    recv_p,
    send_r,
    recv_r,
    send_d,
    recv_d,
    send_h,
    send_w,
    recv_w,
    chain_sem,
    wrap_sem,
):
    planes_all, rows, width = own.shape
    depth = gradk.shape[2]
    count = planes_all // depth
    slabs = groups * members
    grp = lax.axis_index("grp")
    dev = lax.axis_index("dev")
    slab = grp * members + dev
    side = lax.rem(slab, 2)
    step = 2 - 4 * side
    partner = slab + 1 - 2 * side
    follow = lax.rem(slab + slabs + step, slabs)
    other = lax.rem(slab + slabs - step, slabs)
    per = rows // members
    first = jnp.where(side == 0, dev < 2, dev >= members - 2)
    last = jnp.where(side == 0, dev >= members - 2, dev < 2)
    second = jnp.where(side == 0, dev // 2 == 1, dev // 2 == members // 2 - 2)
    ahead_grp = lax.rem(grp + groups + 1 - 2 * side, groups)
    behind_grp = lax.rem(grp + groups - 1 + 2 * side, groups)

    def place(index):
        return (index // members, lax.rem(index, members))

    def signal(semaphore, target):
        pl.semaphore_signal(
            semaphore, inc=1, device_id=target, device_id_type=pl.DeviceIdType.MESH
        )

    barrier = pltpu.get_barrier_semaphore()
    signal(barrier, place(partner))

    @pl.when(jnp.logical_not(last))
    def _():
        signal(barrier, (grp, dev + step))

    @pl.when(jnp.logical_not(first))
    def _():
        signal(barrier, (grp, dev - step))

    @pl.when(last)
    def _():
        signal(barrier, (ahead_grp, dev))

    load = pltpu.make_async_copy(fields_ref, own, own_sem)
    small = (
        pltpu.make_async_copy(mix_hbm, mix_ref, mat_sem.at[0]),
        pltpu.make_async_copy(lap_hbm, lap_ref, mat_sem.at[1]),
    )

    def remote(source, target, send, recv, device):
        return pltpu.make_async_remote_copy(
            src_ref=source,
            dst_ref=target,
            send_sem=send,
            recv_sem=recv,
            device_id=device,
            device_id_type=pl.DeviceIdType.MESH,
        )

    def peer(offset):
        return lax.rem(dev + offset, members)

    chunks = count * depth * HALVES
    final = count - 1
    ahead = min(AHEAD, chunks)
    ring = 2 * ahead

    half = rows // HALVES

    def split(i):
        part = pl.ds(pl.multiple_of(lax.rem(i, HALVES) * half, half), half)
        return i // HALVES, part

    def exchange(i, slot):
        q, part = split(i)
        return remote(
            fields_ref.at[q, part], halo.at[slot, q, part], send_p, recv_p.at[lax.rem(i, ring)], place(partner)
        )

    def relay(i, slot):
        q, part = split(i)
        return remote(
            halo.at[1 - side, q, part],
            halo.at[slot, q, part],
            send_r.at[(q >= planes_all - NEAR).astype(jnp.int32)],
            recv_r.at[q // depth],
            place(follow),
        )

    def detour(planes):
        picked = pl.ds(planes_all - planes, planes)
        return remote(
            fields_ref.at[picked], passing.at[pl.ds(NEAR - planes, planes)], send_d, recv_d, place(other)
        )

    def hand_on(k):
        q = planes_all - k
        return remote(
            passing.at[NEAR - k], halo.at[1 - side, q], send_h.at[k - 1], recv_r.at[q // depth], place(partner)
        )

    def spread(target, source):
        return remote(wloc.at[target], wrecv.at[source], send_w, recv_w, (grp, target))

    pl.semaphore_wait(barrier, jnp.where(first, 2, 3))

    @pl.loop(0, ahead)
    def _(i):
        exchange(i, side).start()

    @pl.when(jnp.logical_not(first))
    def _():
        detour(NEAR).start()

    @pl.when(jnp.logical_not(first))
    def _():
        @pl.when(jnp.logical_not(second))
        def _():
            pl.semaphore_wait(chain_sem, 1)

        @pl.when(last)
        def _():
            signal(wrap_sem, (behind_grp, dev))

        @pl.when(jnp.logical_not(last))
        def _():
            signal(chain_sem, (grp, dev + step))

    load.start()
    for copy in small:
        copy.start()

    @pl.when(last)
    def _():
        pl.semaphore_wait(wrap_sem, 1)

    def advance(i):
        exchange(i, 1 - side).wait_recv()
        q, _ = split(i)

        @pl.when((q < planes_all - NEAR) | (last & (q < planes_all - FAR)))
        def _():
            relay(i, side).start()

        @pl.when(i + ahead < chunks)
        def _():
            exchange(i + ahead, side).start()

    @pl.loop(0, LAG * depth * HALVES)
    def _(i):
        advance(i)

    rhs_ref[...] = jnp.zeros_like(rhs_ref)
    load.wait()
    for copy in small:
        copy.wait()
    for c in range(count):
        for which, table in enumerate((mix_ref, lap_ref)):
            coef_ref[c, which] = jnp.full((8, width), table[c, final], jnp.float32)
    for p in range(depth):
        tail_ref[0, p] = own[final * depth + p]

    def relayed(g):
        part = pl.ds(g * depth, depth)
        remote(halo.at[side, part], halo.at[side, part], send_r.at[0], recv_r.at[g], place(follow)).wait_recv()

    def weyl_local(part):
        tiles = rows // 8
        share = depth * tiles // WEYL_STEPS

        @pl.loop(0, share)
        def _(u):
            t = part * share + u
            p = t // tiles
            start = pl.multiple_of(lax.rem(t, tiles) * 8, 8)
            strip = pl.ds(start, 8)
            curv = [own[(6 + n) * depth + p, strip, :] for n in range(6)]
            lap = [laph[n, p, strip, :] for n in range(6)]
            grad = [[gradk[n, a, p, strip, :] for n in range(6)] for a in range(3)]
            lane = lax.broadcasted_iota(jnp.int32, (8, width), 1)
            row = lax.broadcasted_iota(jnp.int32, (8, width), 0) + start
            layer = jnp.full((8, width), slab * depth + p, jnp.int32)
            along_x = lane.astype(jnp.float32) + (0.5 - 0.5 * width)
            along_y = row.astype(jnp.float32) + (0.5 - 0.5 * rows)
            along_z = layer.astype(jnp.float32) + (0.5 - 0.5 * depth * slabs)
            real, imag = weyl_pair(curv, lap, grad, along_x, along_y, along_z)
            wtmp[0, p, strip, :] = real
            wtmp[1, p, strip, :] = imag

    def process(g, p):
        q = g * depth
        f = own[q + p]
        planes = [halo[0, q], halo[0, q + 1], own[q], own[q + 1], halo[1, q], halo[1, q + 1]]
        zm2, zm1, _, zp1, zp2 = planes[p : p + 5]
        ym1, ym2 = pltpu.roll(f, 1, 0), pltpu.roll(f, 2, 0)
        yp1, yp2 = pltpu.roll(f, rows - 1, 0), pltpu.roll(f, rows - 2, 0)
        xm1, xm2 = pltpu.roll(f, 1, 1), pltpu.roll(f, 2, 1)
        xp1, xp2 = pltpu.roll(f, width - 1, 1), pltpu.roll(f, width - 2, 1)
        near = ((zm1 + zp1) + (ym1 + yp1)) + (xm1 + xp1)
        far_sum = ((zm2 + zp2) + (ym2 + yp2)) + (xm2 + xp2)
        lap = (16.0 * near - far_sum - 90.0 * f) * (1.0 / 12.0)
        lapbuf[p] = lap

        @pl.when(g == final)
        def _():
            tail_ref[1, p] = lap

        gz = (8.0 * (zp1 - zm1) - (zp2 - zm2)) * (1.0 / 12.0)
        gy = (8.0 * (yp1 - ym1) - (yp2 - ym2)) * (1.0 / 12.0)
        gx = (8.0 * (xp1 - xm1) - (xp2 - xm2)) * (1.0 / 12.0)
        rhs_ref[g, p] += own[12 * depth + p] * gz + own[13 * depth + p] * gy + own[14 * depth + p] * gx

        @pl.when(g < 6)
        def _():
            laph[g, p] = lap

        @pl.when(jnp.logical_and(g >= 6, g < 12))
        def _():
            gradk[g - 6, 0, p] = gx
            gradk[g - 6, 1, p] = gy
            gradk[g - 6, 2, p] = gz

        @pl.loop(0, jnp.where(g == final, 0, rows // STRIP))
        def _(t):
            strip = pl.ds(pl.multiple_of(t * STRIP, STRIP), STRIP)
            f = own[q + p, strip, :]
            lap = lapbuf[p, strip, :]
            for c in range(count):
                rhs_ref[c, p, strip, :] += mix_ref[c, g] * f + lap_ref[c, g] * lap

    @pl.loop(0, count)
    def _(g):
        more = g + LAG < count

        @pl.when(more)
        def _():
            for k in range(HALVES):
                advance((g + LAG) * depth * HALVES + k)

        relayed(g)
        process(g, 0)

        @pl.when(more)
        def _():
            for k in range(HALVES):
                advance((g + LAG) * depth * HALVES + HALVES + k)

        process(g, 1)

        @pl.when((g == LEAVE) & first)
        def _():
            detour(FAR).start()

        @pl.when((g == PASS) & last)
        def _():
            detour(FAR).wait_recv()
            for k in range(FAR, 0, -1):
                hand_on(k).start()

        @pl.when((g == PASS) & jnp.logical_not(last))
        def _():
            detour(NEAR).wait_recv()
            for k in range(NEAR, 0, -1):
                hand_on(k).start()

        @pl.when(jnp.logical_and(g >= 11, g < 11 + WEYL_STEPS))
        def _():
            weyl_local(g - 11)

        @pl.when(g == 11 + WEYL_STEPS)
        def _():
            for m in range(members):
                wloc[m] = wtmp[:, :, m * per : (m + 1) * per, :]
            wrecv[dev] = wloc[dev]

        @pl.when(g == 12 + WEYL_STEPS)
        def _():
            for offset in range(1, members):
                spread(peer(offset), dev).start()

    others = pl.ds(0, members - 1)
    remote(wrecv.at[others], wrecv.at[others], send_w, recv_w, (grp, dev)).wait_recv()
    remote(wloc.at[others], wloc.at[others], send_w, recv_w, (grp, dev)).wait_send()
    remote(own, halo.at[0], send_p, recv_p.at[0], place(partner)).wait_send()
    def totals(planes, semaphore):
        part = pl.ds(0, planes)
        remote(halo.at[0, part], halo.at[0, part], semaphore, recv_r.at[0], place(follow)).wait_send()

    totals(planes_all - NEAR, send_r.at[0])

    @pl.when(last)
    def _():
        totals(NEAR - FAR, send_r.at[1])

    for k in range(NEAR, 0, -1):
        if k <= FAR:
            hand_on(k).wait_send()
        else:

            @pl.when(jnp.logical_not(last))
            def _():
                hand_on(k).wait_send()

    @pl.when(first)
    def _():
        detour(FAR).wait_send()

    @pl.when(jnp.logical_not(first))
    def _():
        detour(NEAR).wait_send()


def finish(members, part_ref, wrecv, tail_ref, coef_ref, rhs_ref, weyl_ref, whole, rhs_sem, weyl_sem):
    count, depth, rows, width = part_ref.shape
    blocks = []
    for source in range(members):
        layers = pl.ds(source * depth, depth)
        blocks.append(
            pltpu.make_async_copy(wrecv.at[source], weyl_ref.at[:, layers], weyl_sem.at[source])
        )
    for block in blocks:
        block.start()

    @pl.loop(0, depth * (rows // STRIP))
    def _(t):
        p = t // (rows // STRIP)
        start = pl.multiple_of(lax.rem(t, rows // STRIP) * STRIP, STRIP)
        strip = pl.ds(start, STRIP)
        f = [tail_ref[0, p, pl.ds(start + 8 * k, 8), :] for k in range(STRIP // 8)]
        lap = [tail_ref[1, p, pl.ds(start + 8 * k, 8), :] for k in range(STRIP // 8)]
        for c in range(count):
            mix, spread = coef_ref[c, 0], coef_ref[c, 1]
            for k in range(STRIP // 8):
                part = pl.ds(start + 8 * k, 8)
                whole[c, p, part, :] = part_ref[c, p, part, :] + (mix * f[k] + spread * lap[k])
        pltpu.make_async_copy(whole.at[:, p, strip], rhs_ref.at[:, p, strip], rhs_sem).start()

    for block in blocks:
        block.wait()
    pltpu.make_async_copy(whole, rhs_ref, rhs_sem).wait()


def per_device(groups, members, fields, mix_matrix, laplace_matrix):
    count, depth, rows, width = fields.shape
    assert depth == 2 and members % 4 == 0
    plane = (rows, width)
    per = rows // members
    vmem = functools.partial(pltpu.VMEM, dtype=jnp.float32)
    dma = pltpu.SemaphoreType.DMA
    in_hbm, in_vmem = pl.BlockSpec(memory_space=pltpu.HBM), pl.BlockSpec(memory_space=pltpu.VMEM)
    share = functools.partial(jax.ShapeDtypeStruct, dtype=jnp.float32)
    pieces = pl.pallas_call(
        functools.partial(kernel, groups, members),
        out_shape=(
            share(fields.shape),
            share((members, 2, depth, per, width)),
            share((2, depth) + plane),
            share((count, 2, 8, width)),
        ),
        in_specs=[in_hbm] * 3,
        out_specs=(in_vmem,) * 4,
        scratch_shapes=[
            vmem((count * depth,) + plane),
            vmem((2, count * depth) + plane),
            vmem((depth,) + plane),
            vmem((6, depth) + plane),
            vmem((6, 3, depth) + plane),
            vmem((2, depth) + plane),
            vmem((members, 2, depth, per, width)),
            vmem((NEAR,) + plane),
            pltpu.SMEM((count, count), jnp.float32),
            pltpu.SMEM((count, count), jnp.float32),
            dma,
            dma((2,)),
            dma,
            dma((2 * min(AHEAD, count * depth * HALVES),)),
            dma((2,)),
            dma((count,)),
            dma,
            dma,
            dma((NEAR,)),
            dma,
            dma,
            pltpu.SemaphoreType.REGULAR,
            pltpu.SemaphoreType.REGULAR,
        ],
        compiler_params=pltpu.CompilerParams(
            collective_id=0, has_side_effects=True, vmem_limit_bytes=32 * 1024 * 1024
        ),
        name="evolve",
    )(
        pltpu.with_memory_space_constraint(fields.reshape((count * depth,) + plane), pltpu.HBM),
        pltpu.with_memory_space_constraint(mix_matrix, pltpu.HBM),
        pltpu.with_memory_space_constraint(laplace_matrix, pltpu.HBM),
    )
    return pl.pallas_call(
        functools.partial(finish, members),
        out_shape=(share(fields.shape), share((2, depth * members, per, width))),
        in_specs=[in_vmem] * 4,
        out_specs=(in_hbm,) * 2,
        scratch_shapes=[vmem((count, depth) + plane), dma, dma((members,))],
        compiler_params=pltpu.CompilerParams(vmem_limit_bytes=8 * 1024 * 1024),
        name="finish",
    )(*pieces)


def solution(mesh):
    groups, members = mesh.shape["grp"], mesh.shape["dev"]
    return jax.shard_map(
        functools.partial(per_device, groups, members),
        mesh=mesh,
        in_specs=(P(None, ("grp", "dev"), None, None), P(), P()),
        out_specs=(P(None, ("grp", "dev"), None, None), P(None, "grp", "dev", None)),
        check_vma=False,
    )
```

```python
import functools

import jax
import jax.numpy as jnp
from jax import lax
from jax.experimental import pallas as pl
from jax.experimental.pallas import tpu as pltpu
from jax.sharding import PartitionSpec as P

AHEAD = 12
LAG = 4
WEYL_STEPS = 4
STRIP = 32
MIX = 64
TAIL = 2
HALVES = 2
NEAR = 2
FAR = 2
LEAVE = 8
PASS = 18
TABLE = ((0, 1, 2), (1, 3, 4), (2, 4, 5))
PAIRS = ((0, 0), (0, 1), (0, 2), (1, 1), (1, 2), (2, 2))


def contract(tensor, left, right):
    total = None
    for first in range(3):
        for second in range(3):
            if left[first] is None or right[second] is None:
                continue
            term = tensor[TABLE[first][second]] * (left[first] * right[second])
            total = term if total is None else total + term
    return total


def weyl_pair(curv, lap, grad, along_x, along_y, along_z):
    trace = curv[0] + curv[3] + curv[5]
    electric = []
    for first, second in PAIRS:
        spot = TABLE[first][second]
        value = -0.5 * lap[spot] - trace * curv[spot]
        for middle in range(3):
            value = value + curv[TABLE[first][middle]] * curv[TABLE[middle][second]]
        electric.append(value)

    def curl(first, second):
        one = (first + 1) % 3
        two = (first + 2) % 3
        return grad[one][TABLE[two][second]] - grad[two][TABLE[one][second]]

    magnetic = [0.5 * (curl(first, second) + curl(second, first)) for first, second in PAIRS]
    square = along_x * along_x + along_y * along_y
    cylinder = jnp.sqrt(square)
    radius = jnp.sqrt(square + along_z * along_z)
    over_cyl = 1.0 / cylinder
    over_rad = 1.0 / radius
    slope = along_z * over_rad * over_cyl
    theta = (slope * along_x, slope * along_y, -cylinder * over_rad)
    phi = (-along_y * over_cyl, along_x * over_cyl, None)
    real = 0.5 * (contract(electric, theta, theta) - contract(electric, phi, phi)) - contract(
        magnetic, theta, phi
    )
    imag = -contract(electric, theta, phi) - 0.5 * (
        contract(magnetic, theta, theta) - contract(magnetic, phi, phi)
    )
    return real, imag


def kernel(
    groups,
    members,
    fields_ref,
    mix_hbm,
    lap_hbm,
    rhs_ref,
    wrecv,
    tail_ref,
    coef_ref,
    own,
    halo,
    lapbuf,
    laph,
    gradk,
    wtmp,
    wloc,
    passing,
    mix_ref,
    lap_ref,
    own_sem,
    mat_sem,
    send_p,
    recv_p,
    send_r,
    recv_r,
    send_d,
    recv_d,
    send_h,
    send_w,
    recv_w,
    chain_sem,
    wrap_sem,
):
    planes_all, rows, width = own.shape
    depth = gradk.shape[2]
    count = planes_all // depth
    slabs = groups * members
    grp = lax.axis_index("grp")
    dev = lax.axis_index("dev")
    slab = grp * members + dev
    side = lax.rem(slab, 2)
    step = 2 - 4 * side
    partner = slab + 1 - 2 * side
    follow = lax.rem(slab + slabs + step, slabs)
    other = lax.rem(slab + slabs - step, slabs)
    per = rows // members
    first = jnp.where(side == 0, dev < 2, dev >= members - 2)
    last = jnp.where(side == 0, dev >= members - 2, dev < 2)
    second = jnp.where(side == 0, dev // 2 == 1, dev // 2 == members // 2 - 2)
    ahead_grp = lax.rem(grp + groups + 1 - 2 * side, groups)
    behind_grp = lax.rem(grp + groups - 1 + 2 * side, groups)

    def place(index):
        return (index // members, lax.rem(index, members))

    def signal(semaphore, target):
        pl.semaphore_signal(
            semaphore, inc=1, device_id=target, device_id_type=pl.DeviceIdType.MESH
        )

    barrier = pltpu.get_barrier_semaphore()
    signal(barrier, place(partner))

    @pl.when(jnp.logical_not(last))
    def _():
        signal(barrier, (grp, dev + step))

    @pl.when(jnp.logical_not(first))
    def _():
        signal(barrier, (grp, dev - step))

    @pl.when(last)
    def _():
        signal(barrier, (ahead_grp, dev))

    load = pltpu.make_async_copy(fields_ref, own, own_sem)
    small = (
        pltpu.make_async_copy(mix_hbm, mix_ref, mat_sem.at[0]),
        pltpu.make_async_copy(lap_hbm, lap_ref, mat_sem.at[1]),
    )

    def remote(source, target, send, recv, device):
        return pltpu.make_async_remote_copy(
            src_ref=source,
            dst_ref=target,
            send_sem=send,
            recv_sem=recv,
            device_id=device,
            device_id_type=pl.DeviceIdType.MESH,
        )

    def peer(offset):
        return lax.rem(dev + offset, members)

    chunks = count * depth * HALVES
    final = count - 1
    ahead = min(AHEAD, chunks)
    ring = 2 * ahead

    half = rows // HALVES

    def split(i):
        part = pl.ds(pl.multiple_of(lax.rem(i, HALVES) * half, half), half)
        return i // HALVES, part

    def exchange(i, slot):
        q, part = split(i)
        return remote(
            fields_ref.at[q, part], halo.at[slot, q, part], send_p, recv_p.at[lax.rem(i, ring)], place(partner)
        )

    def relay(i, slot):
        q, part = split(i)
        return remote(
            halo.at[1 - side, q, part],
            halo.at[slot, q, part],
            send_r.at[(q >= planes_all - NEAR).astype(jnp.int32)],
            recv_r.at[q // depth],
            place(follow),
        )

    def detour(planes):
        picked = pl.ds(planes_all - planes, planes)
        return remote(
            fields_ref.at[picked], passing.at[pl.ds(NEAR - planes, planes)], send_d, recv_d, place(other)
        )

    def hand_on(k):
        q = planes_all - k
        return remote(
            passing.at[NEAR - k], halo.at[1 - side, q], send_h.at[k - 1], recv_r.at[q // depth], place(partner)
        )

    def spread(target, source):
        return remote(wloc.at[target], wrecv.at[source], send_w, recv_w, (grp, target))

    pl.semaphore_wait(barrier, jnp.where(first, 2, 3))

    @pl.loop(0, ahead)
    def _(i):
        exchange(i, side).start()

    @pl.when(jnp.logical_not(first))
    def _():
        detour(NEAR).start()

    @pl.when(jnp.logical_not(first))
    def _():
        @pl.when(jnp.logical_not(second))
        def _():
            pl.semaphore_wait(chain_sem, 1)

        @pl.when(last)
        def _():
            signal(wrap_sem, (behind_grp, dev))

        @pl.when(jnp.logical_not(last))
        def _():
            signal(chain_sem, (grp, dev + step))

    load.start()
    for copy in small:
        copy.start()

    rhs_ref[...] = jnp.zeros_like(rhs_ref)
    load.wait()
    for copy in small:
        copy.wait()
    for c in range(count):
        for k in range(TAIL):
            coef_ref[c, k] = jnp.full((8, width), mix_ref[c, count - TAIL + k], jnp.float32)
            coef_ref[c, TAIL + k] = jnp.full((8, width), lap_ref[c, count - TAIL + k], jnp.float32)
    for k in range(TAIL):
        for p in range(depth):
            tail_ref[k, p] = own[(count - TAIL + k) * depth + p]

    @pl.when(last)
    def _():
        pl.semaphore_wait(wrap_sem, 1)

    def advance(i):
        exchange(i, 1 - side).wait_recv()
        q, _ = split(i)

        @pl.when((q < planes_all - NEAR) | (last & (q < planes_all - FAR)))
        def _():
            relay(i, side).start()

        @pl.when(i + ahead < chunks)
        def _():
            exchange(i + ahead, side).start()

    @pl.loop(0, LAG * depth * HALVES)
    def _(i):
        advance(i)

    def relayed(g):
        part = pl.ds(g * depth, depth)
        remote(halo.at[side, part], halo.at[side, part], send_r.at[0], recv_r.at[g], place(follow)).wait_recv()

    def weyl_local(part):
        tiles = rows // 8
        share = depth * tiles // WEYL_STEPS

        @pl.loop(0, share)
        def _(u):
            t = part * share + u
            p = t // tiles
            start = pl.multiple_of(lax.rem(t, tiles) * 8, 8)
            strip = pl.ds(start, 8)
            curv = [own[(6 + n) * depth + p, strip, :] for n in range(6)]
            lap = [laph[n, p, strip, :] for n in range(6)]
            grad = [[gradk[n, a, p, strip, :] for n in range(6)] for a in range(3)]
            lane = lax.broadcasted_iota(jnp.int32, (8, width), 1)
            row = lax.broadcasted_iota(jnp.int32, (8, width), 0) + start
            layer = jnp.full((8, width), slab * depth + p, jnp.int32)
            along_x = lane.astype(jnp.float32) + (0.5 - 0.5 * width)
            along_y = row.astype(jnp.float32) + (0.5 - 0.5 * rows)
            along_z = layer.astype(jnp.float32) + (0.5 - 0.5 * depth * slabs)
            real, imag = weyl_pair(curv, lap, grad, along_x, along_y, along_z)
            wtmp[0, p, strip, :] = real
            wtmp[1, p, strip, :] = imag

    def process(g, p):
        q = g * depth
        f = own[q + p]
        planes = [halo[0, q], halo[0, q + 1], own[q], own[q + 1], halo[1, q], halo[1, q + 1]]
        zm2, zm1, _, zp1, zp2 = planes[p : p + 5]
        ym1, ym2 = pltpu.roll(f, 1, 0), pltpu.roll(f, 2, 0)
        yp1, yp2 = pltpu.roll(f, rows - 1, 0), pltpu.roll(f, rows - 2, 0)
        xm1, xm2 = pltpu.roll(f, 1, 1), pltpu.roll(f, 2, 1)
        xp1, xp2 = pltpu.roll(f, width - 1, 1), pltpu.roll(f, width - 2, 1)
        near = ((zm1 + zp1) + (ym1 + yp1)) + (xm1 + xp1)
        far_sum = ((zm2 + zp2) + (ym2 + yp2)) + (xm2 + xp2)
        lap = (16.0 * near - far_sum - 90.0 * f) * (1.0 / 12.0)
        lapbuf[p] = lap

        @pl.when(g >= count - TAIL)
        def _():
            tail_ref[g - (count - 2 * TAIL), p] = lap

        gz = (8.0 * (zp1 - zm1) - (zp2 - zm2)) * (1.0 / 12.0)
        gy = (8.0 * (yp1 - ym1) - (yp2 - ym2)) * (1.0 / 12.0)
        gx = (8.0 * (xp1 - xm1) - (xp2 - xm2)) * (1.0 / 12.0)
        rhs_ref[g, p] += own[12 * depth + p] * gz + own[13 * depth + p] * gy + own[14 * depth + p] * gx

        @pl.when(g < 6)
        def _():
            laph[g, p] = lap

        @pl.when(jnp.logical_and(g >= 6, g < 12))
        def _():
            gradk[g - 6, 0, p] = gx
            gradk[g - 6, 1, p] = gy
            gradk[g - 6, 2, p] = gz

        @pl.loop(0, jnp.where(g >= count - TAIL, 0, rows // MIX))
        def _(t):
            strip = pl.ds(pl.multiple_of(t * MIX, MIX), MIX)
            f = own[q + p, strip, :]
            lap = lapbuf[p, strip, :]
            for c in range(count):
                rhs_ref[c, p, strip, :] += mix_ref[c, g] * f + lap_ref[c, g] * lap

    @pl.loop(0, count)
    def _(g):
        more = g + LAG < count

        @pl.when(more)
        def _():
            for k in range(HALVES):
                advance((g + LAG) * depth * HALVES + k)

        relayed(g)
        process(g, 0)

        @pl.when(more)
        def _():
            for k in range(HALVES):
                advance((g + LAG) * depth * HALVES + HALVES + k)

        process(g, 1)

        @pl.when((g == LEAVE) & first)
        def _():
            detour(FAR).start()

        @pl.when((g == PASS) & last)
        def _():
            detour(FAR).wait_recv()
            for k in range(FAR, 0, -1):
                hand_on(k).start()

        @pl.when((g == PASS) & jnp.logical_not(last))
        def _():
            detour(NEAR).wait_recv()
            for k in range(NEAR, 0, -1):
                hand_on(k).start()

        @pl.when(jnp.logical_and(g >= 11, g < 11 + WEYL_STEPS))
        def _():
            weyl_local(g - 11)

        @pl.when(g == 11 + WEYL_STEPS)
        def _():
            for m in range(members):
                wloc[m] = wtmp[:, :, m * per : (m + 1) * per, :]
            wrecv[dev] = wloc[dev]

        @pl.when(g == 12 + WEYL_STEPS)
        def _():
            for offset in range(1, members):
                spread(peer(offset), dev).start()

    others = pl.ds(0, members - 1)
    remote(wrecv.at[others], wrecv.at[others], send_w, recv_w, (grp, dev)).wait_recv()
    remote(wloc.at[others], wloc.at[others], send_w, recv_w, (grp, dev)).wait_send()
    remote(own, halo.at[0], send_p, recv_p.at[0], place(partner)).wait_send()
    def totals(planes, semaphore):
        part = pl.ds(0, planes)
        remote(halo.at[0, part], halo.at[0, part], semaphore, recv_r.at[0], place(follow)).wait_send()

    totals(planes_all - NEAR, send_r.at[0])

    @pl.when(last)
    def _():
        totals(NEAR - FAR, send_r.at[1])

    for k in range(NEAR, 0, -1):
        if k <= FAR:
            hand_on(k).wait_send()
        else:

            @pl.when(jnp.logical_not(last))
            def _():
                hand_on(k).wait_send()

    @pl.when(first)
    def _():
        detour(FAR).wait_send()

    @pl.when(jnp.logical_not(first))
    def _():
        detour(NEAR).wait_send()


def finish(members, part_ref, wrecv, tail_ref, coef_ref, rhs_ref, weyl_ref, whole, rhs_sem, weyl_sem):
    count, depth, rows, width = part_ref.shape
    blocks = []
    for source in range(members):
        layers = pl.ds(source * depth, depth)
        blocks.append(
            pltpu.make_async_copy(wrecv.at[source], weyl_ref.at[:, layers], weyl_sem.at[source])
        )
    for block in blocks:
        block.start()

    @pl.loop(0, depth * (rows // STRIP))
    def _(t):
        p = t // (rows // STRIP)
        start = pl.multiple_of(lax.rem(t, rows // STRIP) * STRIP, STRIP)
        strip = pl.ds(start, STRIP)
        terms = [
            [tail_ref[k, p, pl.ds(start + 8 * r, 8), :] for r in range(STRIP // 8)] for k in range(2 * TAIL)
        ]
        for c in range(count):
            coefs = [coef_ref[c, k] for k in range(2 * TAIL)]
            for r in range(STRIP // 8):
                part = pl.ds(start + 8 * r, 8)
                value = part_ref[c, p, part, :]
                for k in range(2 * TAIL):
                    value = value + coefs[k] * terms[k][r]
                whole[c, p, part, :] = value
        pltpu.make_async_copy(whole.at[:, p, strip], rhs_ref.at[:, p, strip], rhs_sem).start()

    for block in blocks:
        block.wait()
    pltpu.make_async_copy(whole, rhs_ref, rhs_sem).wait()


def per_device(groups, members, fields, mix_matrix, laplace_matrix):
    count, depth, rows, width = fields.shape
    assert depth == 2 and members % 4 == 0
    plane = (rows, width)
    per = rows // members
    vmem = functools.partial(pltpu.VMEM, dtype=jnp.float32)
    dma = pltpu.SemaphoreType.DMA
    in_hbm, in_vmem = pl.BlockSpec(memory_space=pltpu.HBM), pl.BlockSpec(memory_space=pltpu.VMEM)
    share = functools.partial(jax.ShapeDtypeStruct, dtype=jnp.float32)
    pieces = pl.pallas_call(
        functools.partial(kernel, groups, members),
        out_shape=(
            share(fields.shape),
            share((members, 2, depth, per, width)),
            share((2 * TAIL, depth) + plane),
            share((count, 2 * TAIL, 8, width)),
        ),
        in_specs=[in_hbm] * 3,
        out_specs=(in_vmem,) * 4,
        scratch_shapes=[
            vmem((count * depth,) + plane),
            vmem((2, count * depth) + plane),
            vmem((depth,) + plane),
            vmem((6, depth) + plane),
            vmem((6, 3, depth) + plane),
            vmem((2, depth) + plane),
            vmem((members, 2, depth, per, width)),
            vmem((NEAR,) + plane),
            pltpu.SMEM((count, count), jnp.float32),
            pltpu.SMEM((count, count), jnp.float32),
            dma,
            dma((2,)),
            dma,
            dma((2 * min(AHEAD, count * depth * HALVES),)),
            dma((2,)),
            dma((count,)),
            dma,
            dma,
            dma((NEAR,)),
            dma,
            dma,
            pltpu.SemaphoreType.REGULAR,
            pltpu.SemaphoreType.REGULAR,
        ],
        compiler_params=pltpu.CompilerParams(
            collective_id=0, has_side_effects=True, vmem_limit_bytes=32 * 1024 * 1024
        ),
        name="evolve",
    )(
        pltpu.with_memory_space_constraint(fields.reshape((count * depth,) + plane), pltpu.HBM),
        pltpu.with_memory_space_constraint(mix_matrix, pltpu.HBM),
        pltpu.with_memory_space_constraint(laplace_matrix, pltpu.HBM),
    )
    return pl.pallas_call(
        functools.partial(finish, members),
        out_shape=(share(fields.shape), share((2, depth * members, per, width))),
        in_specs=[in_vmem] * 4,
        out_specs=(in_hbm,) * 2,
        scratch_shapes=[vmem((count, depth) + plane), dma, dma((members,))],
        compiler_params=pltpu.CompilerParams(vmem_limit_bytes=8 * 1024 * 1024),
        name="finish",
    )(*pieces)


def solution(mesh):
    groups, members = mesh.shape["grp"], mesh.shape["dev"]
    return jax.shard_map(
        functools.partial(per_device, groups, members),
        mesh=mesh,
        in_specs=(P(None, ("grp", "dev"), None, None), P(), P()),
        out_specs=(P(None, ("grp", "dev"), None, None), P(None, "grp", "dev", None)),
        check_vma=False,
    )
```

```python
import functools

import jax
import jax.numpy as jnp
from jax import lax
from jax.experimental import pallas as pl
from jax.experimental.pallas import tpu as pltpu
from jax.sharding import PartitionSpec as P

AHEAD = 12
LAG = 4
WEYL_STEPS = 4
SPREAD_EVEN = 16
SPREAD_ODD = 20
STRIP = 32
MIX = 64
TAIL = 2
HALVES = 2
NEAR = 2
FAR = 2
LEAVE = 8
PASS = 18
TABLE = ((0, 1, 2), (1, 3, 4), (2, 4, 5))
PAIRS = ((0, 0), (0, 1), (0, 2), (1, 1), (1, 2), (2, 2))


def contract(tensor, left, right):
    total = None
    for first in range(3):
        for second in range(3):
            if left[first] is None or right[second] is None:
                continue
            term = tensor[TABLE[first][second]] * (left[first] * right[second])
            total = term if total is None else total + term
    return total


def weyl_pair(curv, lap, grad, along_x, along_y, along_z):
    trace = curv[0] + curv[3] + curv[5]
    electric = []
    for first, second in PAIRS:
        spot = TABLE[first][second]
        value = -0.5 * lap[spot] - trace * curv[spot]
        for middle in range(3):
            value = value + curv[TABLE[first][middle]] * curv[TABLE[middle][second]]
        electric.append(value)

    def curl(first, second):
        one = (first + 1) % 3
        two = (first + 2) % 3
        return grad[one][TABLE[two][second]] - grad[two][TABLE[one][second]]

    magnetic = [0.5 * (curl(first, second) + curl(second, first)) for first, second in PAIRS]
    square = along_x * along_x + along_y * along_y
    cylinder = jnp.sqrt(square)
    radius = jnp.sqrt(square + along_z * along_z)
    over_cyl = 1.0 / cylinder
    over_rad = 1.0 / radius
    slope = along_z * over_rad * over_cyl
    theta = (slope * along_x, slope * along_y, -cylinder * over_rad)
    phi = (-along_y * over_cyl, along_x * over_cyl, None)
    real = 0.5 * (contract(electric, theta, theta) - contract(electric, phi, phi)) - contract(
        magnetic, theta, phi
    )
    imag = -contract(electric, theta, phi) - 0.5 * (
        contract(magnetic, theta, theta) - contract(magnetic, phi, phi)
    )
    return real, imag


def kernel(
    groups,
    members,
    fields_ref,
    mix_hbm,
    lap_hbm,
    rhs_ref,
    wrecv,
    tail_ref,
    coef_ref,
    own,
    halo,
    lapbuf,
    laph,
    gradk,
    wtmp,
    wloc,
    passing,
    mix_ref,
    lap_ref,
    own_sem,
    mat_sem,
    send_p,
    recv_p,
    send_r,
    recv_r,
    send_d,
    recv_d,
    send_h,
    send_w,
    recv_w,
    chain_sem,
    wrap_sem,
):
    planes_all, rows, width = own.shape
    depth = gradk.shape[2]
    count = planes_all // depth
    slabs = groups * members
    grp = lax.axis_index("grp")
    dev = lax.axis_index("dev")
    slab = grp * members + dev
    side = lax.rem(slab, 2)
    step = 2 - 4 * side
    partner = slab + 1 - 2 * side
    follow = lax.rem(slab + slabs + step, slabs)
    other = lax.rem(slab + slabs - step, slabs)
    per = rows // members
    first = jnp.where(side == 0, dev < 2, dev >= members - 2)
    last = jnp.where(side == 0, dev >= members - 2, dev < 2)
    second = jnp.where(side == 0, dev // 2 == 1, dev // 2 == members // 2 - 2)
    ahead_grp = lax.rem(grp + groups + 1 - 2 * side, groups)
    behind_grp = lax.rem(grp + groups - 1 + 2 * side, groups)

    def place(index):
        return (index // members, lax.rem(index, members))

    def signal(semaphore, target):
        pl.semaphore_signal(
            semaphore, inc=1, device_id=target, device_id_type=pl.DeviceIdType.MESH
        )

    barrier = pltpu.get_barrier_semaphore()
    signal(barrier, place(partner))

    @pl.when(jnp.logical_not(last))
    def _():
        signal(barrier, (grp, dev + step))

    @pl.when(jnp.logical_not(first))
    def _():
        signal(barrier, (grp, dev - step))

    @pl.when(last)
    def _():
        signal(barrier, (ahead_grp, dev))

    load = pltpu.make_async_copy(fields_ref, own, own_sem)
    small = (
        pltpu.make_async_copy(mix_hbm, mix_ref, mat_sem.at[0]),
        pltpu.make_async_copy(lap_hbm, lap_ref, mat_sem.at[1]),
    )

    def remote(source, target, send, recv, device):
        return pltpu.make_async_remote_copy(
            src_ref=source,
            dst_ref=target,
            send_sem=send,
            recv_sem=recv,
            device_id=device,
            device_id_type=pl.DeviceIdType.MESH,
        )

    def peer(offset):
        return lax.rem(dev + offset, members)

    chunks = count * depth * HALVES
    final = count - 1
    ahead = min(AHEAD, chunks)
    ring = 2 * ahead

    half = rows // HALVES

    def split(i):
        part = pl.ds(pl.multiple_of(lax.rem(i, HALVES) * half, half), half)
        return i // HALVES, part

    def exchange(i, slot):
        q, part = split(i)
        return remote(
            fields_ref.at[q, part], halo.at[slot, q, part], send_p, recv_p.at[lax.rem(i, ring)], place(partner)
        )

    def relay(i, slot):
        q, part = split(i)
        return remote(
            halo.at[1 - side, q, part],
            halo.at[slot, q, part],
            send_r.at[(q >= planes_all - NEAR).astype(jnp.int32)],
            recv_r.at[q // depth],
            place(follow),
        )

    def detour(planes):
        picked = pl.ds(planes_all - planes, planes)
        return remote(
            fields_ref.at[picked], passing.at[pl.ds(NEAR - planes, planes)], send_d, recv_d, place(other)
        )

    def hand_on(k):
        q = planes_all - k
        return remote(
            passing.at[NEAR - k], halo.at[1 - side, q], send_h.at[k - 1], recv_r.at[q // depth], place(partner)
        )

    def spread(target, source):
        return remote(wloc.at[target], wrecv.at[source], send_w, recv_w, (grp, target))

    pl.semaphore_wait(barrier, jnp.where(first, 2, 3))

    @pl.loop(0, ahead)
    def _(i):
        exchange(i, side).start()

    @pl.when(jnp.logical_not(first))
    def _():
        detour(NEAR).start()

    @pl.when(jnp.logical_not(first))
    def _():
        @pl.when(jnp.logical_not(second))
        def _():
            pl.semaphore_wait(chain_sem, 1)

        @pl.when(last)
        def _():
            signal(wrap_sem, (behind_grp, dev))

        @pl.when(jnp.logical_not(last))
        def _():
            signal(chain_sem, (grp, dev + step))

    load.start()
    for copy in small:
        copy.start()

    rhs_ref[...] = jnp.zeros_like(rhs_ref)
    load.wait()
    for copy in small:
        copy.wait()
    for c in range(count):
        for k in range(TAIL):
            coef_ref[c, k] = jnp.full((8, width), mix_ref[c, count - TAIL + k], jnp.float32)
            coef_ref[c, TAIL + k] = jnp.full((8, width), lap_ref[c, count - TAIL + k], jnp.float32)
    for k in range(TAIL):
        for p in range(depth):
            tail_ref[k, p] = own[(count - TAIL + k) * depth + p]

    @pl.when(last)
    def _():
        pl.semaphore_wait(wrap_sem, 1)

    def advance(i):
        exchange(i, 1 - side).wait_recv()
        q, _ = split(i)

        @pl.when((q < planes_all - NEAR) | (last & (q < planes_all - FAR)))
        def _():
            relay(i, side).start()

        @pl.when(i + ahead < chunks)
        def _():
            exchange(i + ahead, side).start()

    @pl.loop(0, LAG * depth * HALVES)
    def _(i):
        advance(i)

    def relayed(g):
        part = pl.ds(g * depth, depth)
        remote(halo.at[side, part], halo.at[side, part], send_r.at[0], recv_r.at[g], place(follow)).wait_recv()

    def weyl_local(part):
        tiles = rows // 8
        share = depth * tiles // WEYL_STEPS

        @pl.loop(0, share)
        def _(u):
            t = part * share + u
            p = t // tiles
            start = pl.multiple_of(lax.rem(t, tiles) * 8, 8)
            strip = pl.ds(start, 8)
            curv = [own[(6 + n) * depth + p, strip, :] for n in range(6)]
            lap = [laph[n, p, strip, :] for n in range(6)]
            grad = [[gradk[n, a, p, strip, :] for n in range(6)] for a in range(3)]
            lane = lax.broadcasted_iota(jnp.int32, (8, width), 1)
            row = lax.broadcasted_iota(jnp.int32, (8, width), 0) + start
            layer = jnp.full((8, width), slab * depth + p, jnp.int32)
            along_x = lane.astype(jnp.float32) + (0.5 - 0.5 * width)
            along_y = row.astype(jnp.float32) + (0.5 - 0.5 * rows)
            along_z = layer.astype(jnp.float32) + (0.5 - 0.5 * depth * slabs)
            real, imag = weyl_pair(curv, lap, grad, along_x, along_y, along_z)
            wtmp[0, p, strip, :] = real
            wtmp[1, p, strip, :] = imag

    def stencil(f, planes, p):
        zm2, zm1, _, zp1, zp2 = planes[p : p + 5]
        ym1, ym2 = pltpu.roll(f, 1, 0), pltpu.roll(f, 2, 0)
        yp1, yp2 = pltpu.roll(f, rows - 1, 0), pltpu.roll(f, rows - 2, 0)
        xm1, xm2 = pltpu.roll(f, 1, 1), pltpu.roll(f, 2, 1)
        xp1, xp2 = pltpu.roll(f, width - 1, 1), pltpu.roll(f, width - 2, 1)
        near = ((zm1 + zp1) + (ym1 + yp1)) + (xm1 + xp1)
        far_sum = ((zm2 + zp2) + (ym2 + yp2)) + (xm2 + xp2)
        lap = (16.0 * near - far_sum - 90.0 * f) * (1.0 / 12.0)
        gz = (8.0 * (zp1 - zm1) - (zp2 - zm2)) * (1.0 / 12.0)
        gy = (8.0 * (yp1 - ym1) - (yp2 - ym2)) * (1.0 / 12.0)
        gx = (8.0 * (xp1 - xm1) - (xp2 - xm2)) * (1.0 / 12.0)
        return lap, gx, gy, gz

    def process(g, p):
        q = g * depth
        planes = [halo[0, q], halo[0, q + 1], own[q], own[q + 1], halo[1, q], halo[1, q + 1]]
        lap, gx, gy, gz = stencil(own[q + p], planes, p)
        lapbuf[p] = lap
        rhs_ref[g, p] += own[12 * depth + p] * gz + own[13 * depth + p] * gy + own[14 * depth + p] * gx

        @pl.when(g < 6)
        def _():
            laph[g, p] = lap

        @pl.when(jnp.logical_and(g >= 6, g < 12))
        def _():
            gradk[g - 6, 0, p] = gx
            gradk[g - 6, 1, p] = gy
            gradk[g - 6, 2, p] = gz

        @pl.loop(0, rows // MIX)
        def _(t):
            strip = pl.ds(pl.multiple_of(t * MIX, MIX), MIX)
            f = own[q + p, strip, :]
            lap = lapbuf[p, strip, :]
            for c in range(count):
                rhs_ref[c, p, strip, :] += mix_ref[c, g] * f + lap_ref[c, g] * lap

    def without_far(g, p):
        q = g * depth
        zero = jnp.zeros(own.shape[1:], jnp.float32)
        for parity in range(2):

            @pl.when(side == parity)
            def _():
                low = [zero] * depth if parity == 0 else [halo[0, q + k] for k in range(depth)]
                high = [zero] * depth if parity == 1 else [halo[1, q + k] for k in range(depth)]
                planes = low + [own[q + k] for k in range(depth)] + high
                lap, gx, gy, gz = stencil(own[q + p], planes, p)
                tail_ref[g - (count - 2 * TAIL), p] = lap
                rhs_ref[g, p] += (
                    own[12 * depth + p] * gz + own[13 * depth + p] * gy + own[14 * depth + p] * gx
                )

    def far_share(g, p):
        q = g * depth
        for parity in range(2):

            @pl.when(side == parity)
            def _():
                away = depth - 1 - p if parity == 1 else p
                sign = 1.0 if parity == 1 else -1.0
                near, beyond = (q, q + 1) if parity == 1 else (q + 1, q)
                if away == 0:
                    one, two = halo[parity, near], halo[parity, beyond]
                    lap = (16.0 * one - two) * (1.0 / 12.0)
                    gz = (8.0 * one - two) * (sign / 12.0)
                else:
                    two = halo[parity, near]
                    lap = two * (-1.0 / 12.0)
                    gz = two * (-sign / 12.0)
                tail_ref[g - (count - 2 * TAIL), p] += lap
                rhs_ref[g, p] += own[12 * depth + p] * gz

    @pl.loop(0, count - TAIL)
    def _(g):
        more = g + LAG < count

        @pl.when(more)
        def _():
            for k in range(HALVES):
                advance((g + LAG) * depth * HALVES + k)

        relayed(g)
        process(g, 0)

        @pl.when(more)
        def _():
            for k in range(HALVES):
                advance((g + LAG) * depth * HALVES + HALVES + k)

        process(g, 1)

        @pl.when((g == LEAVE) & first)
        def _():
            detour(FAR).start()

        @pl.when((g == PASS) & last)
        def _():
            detour(FAR).wait_recv()
            for k in range(FAR, 0, -1):
                hand_on(k).start()

        @pl.when((g == PASS) & jnp.logical_not(last))
        def _():
            detour(NEAR).wait_recv()
            for k in range(NEAR, 0, -1):
                hand_on(k).start()

        @pl.when(jnp.logical_and(g >= 11, g < 11 + WEYL_STEPS))
        def _():
            weyl_local(g - 11)

        @pl.when(g == 11 + WEYL_STEPS)
        def _():
            for m in range(members):
                wloc[m] = wtmp[:, :, m * per : (m + 1) * per, :]
            wrecv[dev] = wloc[dev]

        @pl.when(g == jnp.where(lax.rem(grp, 2) == 0, SPREAD_EVEN, SPREAD_ODD))
        def _():
            for offset in range(1, members):
                spread(peer(offset), dev).start()

    for g in range(count - TAIL, count):
        for p in range(depth):
            without_far(g, p)
    for g in range(count - 1, count - TAIL - 1, -1):
        relayed(g)
        for p in range(depth):
            far_share(g, p)

    others = pl.ds(0, members - 1)
    remote(wrecv.at[others], wrecv.at[others], send_w, recv_w, (grp, dev)).wait_recv()
    remote(wloc.at[others], wloc.at[others], send_w, recv_w, (grp, dev)).wait_send()
    remote(own, halo.at[0], send_p, recv_p.at[0], place(partner)).wait_send()
    def totals(planes, semaphore):
        part = pl.ds(0, planes)
        remote(halo.at[0, part], halo.at[0, part], semaphore, recv_r.at[0], place(follow)).wait_send()

    totals(planes_all - NEAR, send_r.at[0])

    @pl.when(last)
    def _():
        totals(NEAR - FAR, send_r.at[1])

    for k in range(NEAR, 0, -1):
        if k <= FAR:
            hand_on(k).wait_send()
        else:

            @pl.when(jnp.logical_not(last))
            def _():
                hand_on(k).wait_send()

    @pl.when(first)
    def _():
        detour(FAR).wait_send()

    @pl.when(jnp.logical_not(first))
    def _():
        detour(NEAR).wait_send()


def finish(members, part_ref, wrecv, tail_ref, coef_ref, rhs_ref, weyl_ref, whole, rhs_sem, weyl_sem):
    count, depth, rows, width = part_ref.shape
    blocks = []
    for source in range(members):
        layers = pl.ds(source * depth, depth)
        blocks.append(
            pltpu.make_async_copy(wrecv.at[source], weyl_ref.at[:, layers], weyl_sem.at[source])
        )
    for block in blocks:
        block.start()

    @pl.loop(0, depth * (rows // STRIP))
    def _(t):
        p = t // (rows // STRIP)
        start = pl.multiple_of(lax.rem(t, rows // STRIP) * STRIP, STRIP)
        strip = pl.ds(start, STRIP)
        terms = [
            [tail_ref[k, p, pl.ds(start + 8 * r, 8), :] for r in range(STRIP // 8)] for k in range(2 * TAIL)
        ]
        for c in range(count):
            coefs = [coef_ref[c, k] for k in range(2 * TAIL)]
            for r in range(STRIP // 8):
                part = pl.ds(start + 8 * r, 8)
                value = part_ref[c, p, part, :]
                for k in range(2 * TAIL):
                    value = value + coefs[k] * terms[k][r]
                whole[c, p, part, :] = value
        pltpu.make_async_copy(whole.at[:, p, strip], rhs_ref.at[:, p, strip], rhs_sem).start()

    for block in blocks:
        block.wait()
    pltpu.make_async_copy(whole, rhs_ref, rhs_sem).wait()


def per_device(groups, members, fields, mix_matrix, laplace_matrix):
    count, depth, rows, width = fields.shape
    assert depth == 2 and members % 4 == 0
    plane = (rows, width)
    per = rows // members
    vmem = functools.partial(pltpu.VMEM, dtype=jnp.float32)
    dma = pltpu.SemaphoreType.DMA
    in_hbm, in_vmem = pl.BlockSpec(memory_space=pltpu.HBM), pl.BlockSpec(memory_space=pltpu.VMEM)
    share = functools.partial(jax.ShapeDtypeStruct, dtype=jnp.float32)
    pieces = pl.pallas_call(
        functools.partial(kernel, groups, members),
        out_shape=(
            share(fields.shape),
            share((members, 2, depth, per, width)),
            share((2 * TAIL, depth) + plane),
            share((count, 2 * TAIL, 8, width)),
        ),
        in_specs=[in_hbm] * 3,
        out_specs=(in_vmem,) * 4,
        scratch_shapes=[
            vmem((count * depth,) + plane),
            vmem((2, count * depth) + plane),
            vmem((depth,) + plane),
            vmem((6, depth) + plane),
            vmem((6, 3, depth) + plane),
            vmem((2, depth) + plane),
            vmem((members, 2, depth, per, width)),
            vmem((NEAR,) + plane),
            pltpu.SMEM((count, count), jnp.float32),
            pltpu.SMEM((count, count), jnp.float32),
            dma,
            dma((2,)),
            dma,
            dma((2 * min(AHEAD, count * depth * HALVES),)),
            dma((2,)),
            dma((count,)),
            dma,
            dma,
            dma((NEAR,)),
            dma,
            dma,
            pltpu.SemaphoreType.REGULAR,
            pltpu.SemaphoreType.REGULAR,
        ],
        compiler_params=pltpu.CompilerParams(
            collective_id=0, has_side_effects=True, vmem_limit_bytes=32 * 1024 * 1024
        ),
        name="evolve",
    )(
        pltpu.with_memory_space_constraint(fields.reshape((count * depth,) + plane), pltpu.HBM),
        pltpu.with_memory_space_constraint(mix_matrix, pltpu.HBM),
        pltpu.with_memory_space_constraint(laplace_matrix, pltpu.HBM),
    )
    return pl.pallas_call(
        functools.partial(finish, members),
        out_shape=(share(fields.shape), share((2, depth * members, per, width))),
        in_specs=[in_vmem] * 4,
        out_specs=(in_hbm,) * 2,
        scratch_shapes=[vmem((count, depth) + plane), dma, dma((members,))],
        compiler_params=pltpu.CompilerParams(vmem_limit_bytes=8 * 1024 * 1024),
        name="finish",
    )(*pieces)


def solution(mesh):
    groups, members = mesh.shape["grp"], mesh.shape["dev"]
    return jax.shard_map(
        functools.partial(per_device, groups, members),
        mesh=mesh,
        in_specs=(P(None, ("grp", "dev"), None, None), P(), P()),
        out_specs=(P(None, ("grp", "dev"), None, None), P(None, "grp", "dev", None)),
        check_vma=False,
    )
```

```python
import functools

import jax
import jax.numpy as jnp
from jax import lax
from jax.experimental import pallas as pl
from jax.experimental.pallas import tpu as pltpu
from jax.sharding import PartitionSpec as P

AHEAD = 6
LAG = 4
WEYL_STEPS = 4
SPREAD_EVEN = 16
SPREAD_ODD = 20
STRIP = 16
MIX = 64
TAIL = 2
HALVES = 2
NEAR = 2
FAR = 2
LEAVE = 8
PASS = 18
TABLE = ((0, 1, 2), (1, 3, 4), (2, 4, 5))
PAIRS = ((0, 0), (0, 1), (0, 2), (1, 1), (1, 2), (2, 2))


def contract(tensor, left, right):
    total = None
    for first in range(3):
        for second in range(3):
            if left[first] is None or right[second] is None:
                continue
            term = tensor[TABLE[first][second]] * (left[first] * right[second])
            total = term if total is None else total + term
    return total


def weyl_pair(curv, lap, grad, along_x, along_y, along_z):
    trace = curv[0] + curv[3] + curv[5]
    electric = []
    for first, second in PAIRS:
        spot = TABLE[first][second]
        value = -0.5 * lap[spot] - trace * curv[spot]
        for middle in range(3):
            value = value + curv[TABLE[first][middle]] * curv[TABLE[middle][second]]
        electric.append(value)

    def curl(first, second):
        one = (first + 1) % 3
        two = (first + 2) % 3
        return grad[one][TABLE[two][second]] - grad[two][TABLE[one][second]]

    magnetic = [0.5 * (curl(first, second) + curl(second, first)) for first, second in PAIRS]
    square = along_x * along_x + along_y * along_y
    cylinder = jnp.sqrt(square)
    radius = jnp.sqrt(square + along_z * along_z)
    over_cyl = 1.0 / cylinder
    over_rad = 1.0 / radius
    slope = along_z * over_rad * over_cyl
    theta = (slope * along_x, slope * along_y, -cylinder * over_rad)
    phi = (-along_y * over_cyl, along_x * over_cyl, None)
    real = 0.5 * (contract(electric, theta, theta) - contract(electric, phi, phi)) - contract(
        magnetic, theta, phi
    )
    imag = -contract(electric, theta, phi) - 0.5 * (
        contract(magnetic, theta, theta) - contract(magnetic, phi, phi)
    )
    return real, imag


def kernel(
    groups,
    members,
    fields_ref,
    mix_hbm,
    lap_hbm,
    rhs_ref,
    wrecv,
    tail_ref,
    coef_ref,
    own,
    halo,
    lapbuf,
    laph,
    gradk,
    wtmp,
    wloc,
    passing,
    mix_ref,
    lap_ref,
    own_sem,
    mat_sem,
    send_p,
    recv_p,
    send_r,
    recv_r,
    send_d,
    recv_d,
    send_h,
    send_w,
    recv_w,
    chain_sem,
    wrap_sem,
):
    planes_all, rows, width = own.shape
    depth = gradk.shape[2]
    count = planes_all // depth
    slabs = groups * members
    grp = lax.axis_index("grp")
    dev = lax.axis_index("dev")
    slab = grp * members + dev
    side = lax.rem(slab, 2)
    step = 2 - 4 * side
    partner = slab + 1 - 2 * side
    follow = lax.rem(slab + slabs + step, slabs)
    other = lax.rem(slab + slabs - step, slabs)
    per = rows // members
    first = jnp.where(side == 0, dev < 2, dev >= members - 2)
    last = jnp.where(side == 0, dev >= members - 2, dev < 2)
    second = jnp.where(side == 0, dev // 2 == 1, dev // 2 == members // 2 - 2)
    ahead_grp = lax.rem(grp + groups + 1 - 2 * side, groups)
    behind_grp = lax.rem(grp + groups - 1 + 2 * side, groups)

    def place(index):
        return (index // members, lax.rem(index, members))

    def signal(semaphore, target):
        pl.semaphore_signal(
            semaphore, inc=1, device_id=target, device_id_type=pl.DeviceIdType.MESH
        )

    barrier = pltpu.get_barrier_semaphore()
    signal(barrier, place(partner))

    @pl.when(jnp.logical_not(last))
    def _():
        signal(barrier, (grp, dev + step))

    @pl.when(jnp.logical_not(first))
    def _():
        signal(barrier, (grp, dev - step))

    @pl.when(last)
    def _():
        signal(barrier, (ahead_grp, dev))

    load = pltpu.make_async_copy(fields_ref, own, own_sem)
    small = (
        pltpu.make_async_copy(mix_hbm, mix_ref, mat_sem.at[0]),
        pltpu.make_async_copy(lap_hbm, lap_ref, mat_sem.at[1]),
    )

    def remote(source, target, send, recv, device):
        return pltpu.make_async_remote_copy(
            src_ref=source,
            dst_ref=target,
            send_sem=send,
            recv_sem=recv,
            device_id=device,
            device_id_type=pl.DeviceIdType.MESH,
        )

    def peer(offset):
        return lax.rem(dev + offset, members)

    chunks = count * depth * HALVES
    final = count - 1
    ahead = min(AHEAD, chunks)
    ring = 2 * ahead

    half = rows // HALVES

    def split(i):
        part = pl.ds(pl.multiple_of(lax.rem(i, HALVES) * half, half), half)
        return i // HALVES, part

    def exchange(i, slot):
        q, part = split(i)
        return remote(
            fields_ref.at[q, part], halo.at[slot, q, part], send_p, recv_p.at[lax.rem(i, ring)], place(partner)
        )

    def relay(i, slot):
        q, part = split(i)
        return remote(
            halo.at[1 - side, q, part],
            halo.at[slot, q, part],
            send_r.at[(q >= planes_all - NEAR).astype(jnp.int32)],
            recv_r.at[q // depth],
            place(follow),
        )

    def detour(planes):
        picked = pl.ds(planes_all - planes, planes)
        return remote(
            fields_ref.at[picked], passing.at[pl.ds(NEAR - planes, planes)], send_d, recv_d, place(other)
        )

    def hand_on(k):
        q = planes_all - k
        return remote(
            passing.at[NEAR - k], halo.at[1 - side, q], send_h.at[k - 1], recv_r.at[q // depth], place(partner)
        )

    def spread(target, source):
        return remote(wloc.at[target], wrecv.at[source], send_w, recv_w, (grp, target))

    pl.semaphore_wait(barrier, jnp.where(first, 2, 3))

    @pl.loop(0, ahead)
    def _(i):
        exchange(i, side).start()

    @pl.when(jnp.logical_not(first))
    def _():
        detour(NEAR).start()

    @pl.when(jnp.logical_not(first))
    def _():
        @pl.when(jnp.logical_not(second))
        def _():
            pl.semaphore_wait(chain_sem, 1)

        @pl.when(last)
        def _():
            signal(wrap_sem, (behind_grp, dev))

        @pl.when(jnp.logical_not(last))
        def _():
            signal(chain_sem, (grp, dev + step))

    load.start()
    for copy in small:
        copy.start()

    rhs_ref[...] = jnp.zeros_like(rhs_ref)
    load.wait()
    for copy in small:
        copy.wait()
    for c in range(count):
        for k in range(TAIL):
            coef_ref[c, k] = jnp.full((8, width), mix_ref[c, count - TAIL + k], jnp.float32)
            coef_ref[c, TAIL + k] = jnp.full((8, width), lap_ref[c, count - TAIL + k], jnp.float32)
    for k in range(TAIL):
        for p in range(depth):
            tail_ref[k, p] = own[(count - TAIL + k) * depth + p]

    @pl.when(last)
    def _():
        pl.semaphore_wait(wrap_sem, 1)

    def advance(i):
        exchange(i, 1 - side).wait_recv()
        q, _ = split(i)

        @pl.when((q < planes_all - NEAR) | (last & (q < planes_all - FAR)))
        def _():
            relay(i, side).start()

        @pl.when(i + ahead < chunks)
        def _():
            exchange(i + ahead, side).start()

    @pl.loop(0, LAG * depth * HALVES)
    def _(i):
        advance(i)

    def relayed(g):
        part = pl.ds(g * depth, depth)
        remote(halo.at[side, part], halo.at[side, part], send_r.at[0], recv_r.at[g], place(follow)).wait_recv()

    def weyl_local(part):
        tiles = rows // 8
        share = depth * tiles // WEYL_STEPS

        @pl.loop(0, share)
        def _(u):
            t = part * share + u
            p = t // tiles
            start = pl.multiple_of(lax.rem(t, tiles) * 8, 8)
            strip = pl.ds(start, 8)
            curv = [own[(6 + n) * depth + p, strip, :] for n in range(6)]
            lap = [laph[n, p, strip, :] for n in range(6)]
            grad = [[gradk[n, a, p, strip, :] for n in range(6)] for a in range(3)]
            lane = lax.broadcasted_iota(jnp.int32, (8, width), 1)
            row = lax.broadcasted_iota(jnp.int32, (8, width), 0) + start
            layer = jnp.full((8, width), slab * depth + p, jnp.int32)
            along_x = lane.astype(jnp.float32) + (0.5 - 0.5 * width)
            along_y = row.astype(jnp.float32) + (0.5 - 0.5 * rows)
            along_z = layer.astype(jnp.float32) + (0.5 - 0.5 * depth * slabs)
            real, imag = weyl_pair(curv, lap, grad, along_x, along_y, along_z)
            wtmp[0, p, strip, :] = real
            wtmp[1, p, strip, :] = imag

    def stencil(f, planes, p):
        zm2, zm1, _, zp1, zp2 = planes[p : p + 5]
        ym1, ym2 = pltpu.roll(f, 1, 0), pltpu.roll(f, 2, 0)
        yp1, yp2 = pltpu.roll(f, rows - 1, 0), pltpu.roll(f, rows - 2, 0)
        xm1, xm2 = pltpu.roll(f, 1, 1), pltpu.roll(f, 2, 1)
        xp1, xp2 = pltpu.roll(f, width - 1, 1), pltpu.roll(f, width - 2, 1)
        near = ((zm1 + zp1) + (ym1 + yp1)) + (xm1 + xp1)
        far_sum = ((zm2 + zp2) + (ym2 + yp2)) + (xm2 + xp2)
        lap = (16.0 * near - far_sum - 90.0 * f) * (1.0 / 12.0)
        gz = (8.0 * (zp1 - zm1) - (zp2 - zm2)) * (1.0 / 12.0)
        gy = (8.0 * (yp1 - ym1) - (yp2 - ym2)) * (1.0 / 12.0)
        gx = (8.0 * (xp1 - xm1) - (xp2 - xm2)) * (1.0 / 12.0)
        return lap, gx, gy, gz

    def process(g, p):
        q = g * depth
        planes = [halo[0, q], halo[0, q + 1], own[q], own[q + 1], halo[1, q], halo[1, q + 1]]
        lap, gx, gy, gz = stencil(own[q + p], planes, p)
        lapbuf[p] = lap
        rhs_ref[g, p] += own[12 * depth + p] * gz + own[13 * depth + p] * gy + own[14 * depth + p] * gx

        @pl.when(g < 6)
        def _():
            laph[g, p] = lap

        @pl.when(jnp.logical_and(g >= 6, g < 12))
        def _():
            gradk[g - 6, 0, p] = gx
            gradk[g - 6, 1, p] = gy
            gradk[g - 6, 2, p] = gz

        @pl.loop(0, rows // MIX)
        def _(t):
            strip = pl.ds(pl.multiple_of(t * MIX, MIX), MIX)
            f = own[q + p, strip, :]
            lap = lapbuf[p, strip, :]
            for c in range(count):
                rhs_ref[c, p, strip, :] += mix_ref[c, g] * f + lap_ref[c, g] * lap

    def without_far(g, p):
        q = g * depth
        zero = jnp.zeros(own.shape[1:], jnp.float32)
        for parity in range(2):

            @pl.when(side == parity)
            def _():
                low = [zero] * depth if parity == 0 else [halo[0, q + k] for k in range(depth)]
                high = [zero] * depth if parity == 1 else [halo[1, q + k] for k in range(depth)]
                planes = low + [own[q + k] for k in range(depth)] + high
                lap, gx, gy, gz = stencil(own[q + p], planes, p)
                tail_ref[g - (count - 2 * TAIL), p] = lap
                rhs_ref[g, p] += (
                    own[12 * depth + p] * gz + own[13 * depth + p] * gy + own[14 * depth + p] * gx
                )

    def far_share(g, p):
        q = g * depth
        for parity in range(2):

            @pl.when(side == parity)
            def _():
                away = depth - 1 - p if parity == 1 else p
                sign = 1.0 if parity == 1 else -1.0
                near, beyond = (q, q + 1) if parity == 1 else (q + 1, q)
                if away == 0:
                    one, two = halo[parity, near], halo[parity, beyond]
                    lap = (16.0 * one - two) * (1.0 / 12.0)
                    gz = (8.0 * one - two) * (sign / 12.0)
                else:
                    two = halo[parity, near]
                    lap = two * (-1.0 / 12.0)
                    gz = two * (-sign / 12.0)
                tail_ref[g - (count - 2 * TAIL), p] += lap
                rhs_ref[g, p] += own[12 * depth + p] * gz

    @pl.loop(0, count - TAIL)
    def _(g):
        more = g + LAG < count

        @pl.when(more)
        def _():
            for k in range(HALVES):
                advance((g + LAG) * depth * HALVES + k)

        relayed(g)
        process(g, 0)

        @pl.when(more)
        def _():
            for k in range(HALVES):
                advance((g + LAG) * depth * HALVES + HALVES + k)

        process(g, 1)

        @pl.when((g == LEAVE) & first)
        def _():
            detour(FAR).start()

        @pl.when((g == PASS) & last)
        def _():
            detour(FAR).wait_recv()
            for k in range(FAR, 0, -1):
                hand_on(k).start()

        @pl.when((g == PASS) & jnp.logical_not(last))
        def _():
            detour(NEAR).wait_recv()
            for k in range(NEAR, 0, -1):
                hand_on(k).start()

        @pl.when(jnp.logical_and(g >= 11, g < 11 + WEYL_STEPS))
        def _():
            weyl_local(g - 11)

        @pl.when(g == 11 + WEYL_STEPS)
        def _():
            for m in range(members):
                wloc[m] = wtmp[:, :, m * per : (m + 1) * per, :]
            wrecv[dev] = wloc[dev]

        @pl.when(g == jnp.where(lax.rem(grp, 2) == 0, SPREAD_EVEN, SPREAD_ODD))
        def _():
            for offset in range(1, members):
                spread(peer(offset), dev).start()

    for g in range(count - TAIL, count):
        for p in range(depth):
            without_far(g, p)
    for g in range(count - 1, count - TAIL - 1, -1):
        relayed(g)
        for p in range(depth):
            far_share(g, p)

    others = pl.ds(0, members - 1)
    remote(wrecv.at[others], wrecv.at[others], send_w, recv_w, (grp, dev)).wait_recv()
    remote(wloc.at[others], wloc.at[others], send_w, recv_w, (grp, dev)).wait_send()
    remote(own, halo.at[0], send_p, recv_p.at[0], place(partner)).wait_send()
    def totals(planes, semaphore):
        part = pl.ds(0, planes)
        remote(halo.at[0, part], halo.at[0, part], semaphore, recv_r.at[0], place(follow)).wait_send()

    totals(planes_all - NEAR, send_r.at[0])

    @pl.when(last)
    def _():
        totals(NEAR - FAR, send_r.at[1])

    for k in range(NEAR, 0, -1):
        if k <= FAR:
            hand_on(k).wait_send()
        else:

            @pl.when(jnp.logical_not(last))
            def _():
                hand_on(k).wait_send()

    @pl.when(first)
    def _():
        detour(FAR).wait_send()

    @pl.when(jnp.logical_not(first))
    def _():
        detour(NEAR).wait_send()


def finish(members, part_ref, wrecv, tail_ref, coef_ref, rhs_ref, weyl_ref, whole, rhs_sem, weyl_sem):
    count, depth, rows, width = part_ref.shape
    blocks = []
    for source in range(members):
        layers = pl.ds(source * depth, depth)
        blocks.append(
            pltpu.make_async_copy(wrecv.at[source], weyl_ref.at[:, layers], weyl_sem.at[source])
        )
    for block in blocks:
        block.start()

    @pl.loop(0, depth * (rows // STRIP))
    def _(t):
        p = t // (rows // STRIP)
        start = pl.multiple_of(lax.rem(t, rows // STRIP) * STRIP, STRIP)
        strip = pl.ds(start, STRIP)
        terms = [
            [tail_ref[k, p, pl.ds(start + 8 * r, 8), :] for r in range(STRIP // 8)] for k in range(2 * TAIL)
        ]
        for c in range(count):
            coefs = [coef_ref[c, k] for k in range(2 * TAIL)]
            for r in range(STRIP // 8):
                part = pl.ds(start + 8 * r, 8)
                value = part_ref[c, p, part, :]
                for k in range(2 * TAIL):
                    value = value + coefs[k] * terms[k][r]
                whole[c, p, part, :] = value
        pltpu.make_async_copy(whole.at[:, p, strip], rhs_ref.at[:, p, strip], rhs_sem).start()

    for block in blocks:
        block.wait()
    pltpu.make_async_copy(whole, rhs_ref, rhs_sem).wait()


def per_device(groups, members, fields, mix_matrix, laplace_matrix):
    count, depth, rows, width = fields.shape
    assert depth == 2 and members % 4 == 0
    plane = (rows, width)
    per = rows // members
    vmem = functools.partial(pltpu.VMEM, dtype=jnp.float32)
    dma = pltpu.SemaphoreType.DMA
    in_hbm, in_vmem = pl.BlockSpec(memory_space=pltpu.HBM), pl.BlockSpec(memory_space=pltpu.VMEM)
    share = functools.partial(jax.ShapeDtypeStruct, dtype=jnp.float32)
    pieces = pl.pallas_call(
        functools.partial(kernel, groups, members),
        out_shape=(
            share(fields.shape),
            share((members, 2, depth, per, width)),
            share((2 * TAIL, depth) + plane),
            share((count, 2 * TAIL, 8, width)),
        ),
        in_specs=[in_hbm] * 3,
        out_specs=(in_vmem,) * 4,
        scratch_shapes=[
            vmem((count * depth,) + plane),
            vmem((2, count * depth) + plane),
            vmem((depth,) + plane),
            vmem((6, depth) + plane),
            vmem((6, 3, depth) + plane),
            vmem((2, depth) + plane),
            vmem((members, 2, depth, per, width)),
            vmem((NEAR,) + plane),
            pltpu.SMEM((count, count), jnp.float32),
            pltpu.SMEM((count, count), jnp.float32),
            dma,
            dma((2,)),
            dma,
            dma((2 * min(AHEAD, count * depth * HALVES),)),
            dma((2,)),
            dma((count,)),
            dma,
            dma,
            dma((NEAR,)),
            dma,
            dma,
            pltpu.SemaphoreType.REGULAR,
            pltpu.SemaphoreType.REGULAR,
        ],
        compiler_params=pltpu.CompilerParams(
            collective_id=0, has_side_effects=True, vmem_limit_bytes=32 * 1024 * 1024
        ),
        name="evolve",
    )(
        pltpu.with_memory_space_constraint(fields.reshape((count * depth,) + plane), pltpu.HBM),
        pltpu.with_memory_space_constraint(mix_matrix, pltpu.HBM),
        pltpu.with_memory_space_constraint(laplace_matrix, pltpu.HBM),
    )
    return pl.pallas_call(
        functools.partial(finish, members),
        out_shape=(share(fields.shape), share((2, depth * members, per, width))),
        in_specs=[in_vmem] * 4,
        out_specs=(in_hbm,) * 2,
        scratch_shapes=[vmem((count, depth) + plane), dma, dma((members,))],
        compiler_params=pltpu.CompilerParams(vmem_limit_bytes=8 * 1024 * 1024),
        name="finish",
    )(*pieces)


def solution(mesh):
    groups, members = mesh.shape["grp"], mesh.shape["dev"]
    return jax.shard_map(
        functools.partial(per_device, groups, members),
        mesh=mesh,
        in_specs=(P(None, ("grp", "dev"), None, None), P(), P()),
        out_specs=(P(None, ("grp", "dev"), None, None), P(None, "grp", "dev", None)),
        check_vma=False,
    )
```

```python
import functools

import jax
import jax.numpy as jnp
from jax import lax
from jax.experimental import pallas as pl
from jax.experimental.pallas import tpu as pltpu
from jax.sharding import PartitionSpec as P

AHEAD = 6
LAG = 4
WEYL_STEPS = 4
SPREAD_EVEN = 16
SPREAD_ODD = 20
STRIP = 16
MIX = 64
TAIL = 2
HALVES = 2
NEAR = 2
FAR = 2
LEAVE = 8
PASS = 18
TABLE = ((0, 1, 2), (1, 3, 4), (2, 4, 5))
PAIRS = ((0, 0), (0, 1), (0, 2), (1, 1), (1, 2), (2, 2))


def contract(tensor, left, right):
    total = None
    for first in range(3):
        for second in range(3):
            if left[first] is None or right[second] is None:
                continue
            term = tensor[TABLE[first][second]] * (left[first] * right[second])
            total = term if total is None else total + term
    return total


def weyl_pair(curv, lap, grad, along_x, along_y, along_z):
    trace = curv[0] + curv[3] + curv[5]
    electric = []
    for first, second in PAIRS:
        spot = TABLE[first][second]
        value = -0.5 * lap[spot] - trace * curv[spot]
        for middle in range(3):
            value = value + curv[TABLE[first][middle]] * curv[TABLE[middle][second]]
        electric.append(value)

    def curl(first, second):
        one = (first + 1) % 3
        two = (first + 2) % 3
        return grad[one][TABLE[two][second]] - grad[two][TABLE[one][second]]

    magnetic = [0.5 * (curl(first, second) + curl(second, first)) for first, second in PAIRS]
    square = along_x * along_x + along_y * along_y
    cylinder = jnp.sqrt(square)
    radius = jnp.sqrt(square + along_z * along_z)
    over_cyl = 1.0 / cylinder
    over_rad = 1.0 / radius
    slope = along_z * over_rad * over_cyl
    theta = (slope * along_x, slope * along_y, -cylinder * over_rad)
    phi = (-along_y * over_cyl, along_x * over_cyl, None)
    real = 0.5 * (contract(electric, theta, theta) - contract(electric, phi, phi)) - contract(
        magnetic, theta, phi
    )
    imag = -contract(electric, theta, phi) - 0.5 * (
        contract(magnetic, theta, theta) - contract(magnetic, phi, phi)
    )
    return real, imag


def kernel(
    groups,
    members,
    fields_ref,
    mix_hbm,
    lap_hbm,
    rhs_ref,
    wrecv,
    tail_ref,
    coef_ref,
    own,
    halo,
    lapbuf,
    laph,
    gradk,
    wtmp,
    wloc,
    passing,
    mix_ref,
    lap_ref,
    own_sem,
    mat_sem,
    send_p,
    recv_p,
    send_r,
    recv_r,
    send_d,
    recv_d,
    send_h,
    send_w,
    recv_w,
    chain_sem,
    wrap_sem,
):
    planes_all, rows, width = own.shape
    depth = gradk.shape[2]
    count = planes_all // depth
    slabs = groups * members
    grp = lax.axis_index("grp")
    dev = lax.axis_index("dev")
    slab = grp * members + dev
    side = lax.rem(slab, 2)
    step = 2 - 4 * side
    partner = slab + 1 - 2 * side
    follow = lax.rem(slab + slabs + step, slabs)
    other = lax.rem(slab + slabs - step, slabs)
    per = rows // members
    first = jnp.where(side == 0, dev < 2, dev >= members - 2)
    last = jnp.where(side == 0, dev >= members - 2, dev < 2)
    second = jnp.where(side == 0, dev // 2 == 1, dev // 2 == members // 2 - 2)
    ahead_grp = lax.rem(grp + groups + 1 - 2 * side, groups)
    behind_grp = lax.rem(grp + groups - 1 + 2 * side, groups)

    def place(index):
        return (index // members, lax.rem(index, members))

    def signal(semaphore, target):
        pl.semaphore_signal(
            semaphore, inc=1, device_id=target, device_id_type=pl.DeviceIdType.MESH
        )

    barrier = pltpu.get_barrier_semaphore()
    signal(barrier, place(partner))

    @pl.when(jnp.logical_not(last))
    def _():
        signal(barrier, (grp, dev + step))

    @pl.when(jnp.logical_not(first))
    def _():
        signal(barrier, (grp, dev - step))

    @pl.when(last)
    def _():
        signal(barrier, (ahead_grp, dev))

    load = pltpu.make_async_copy(fields_ref, own, own_sem)
    small = (
        pltpu.make_async_copy(mix_hbm, mix_ref, mat_sem.at[0]),
        pltpu.make_async_copy(lap_hbm, lap_ref, mat_sem.at[1]),
    )

    def remote(source, target, send, recv, device):
        return pltpu.make_async_remote_copy(
            src_ref=source,
            dst_ref=target,
            send_sem=send,
            recv_sem=recv,
            device_id=device,
            device_id_type=pl.DeviceIdType.MESH,
        )

    def peer(offset):
        return lax.rem(dev + offset, members)

    chunks = count * depth * HALVES
    final = count - 1
    ahead = min(AHEAD, chunks)
    ring = 2 * ahead

    half = rows // HALVES

    def split(i):
        part = pl.ds(pl.multiple_of(lax.rem(i, HALVES) * half, half), half)
        return i // HALVES, part

    def exchange(i, slot):
        q, part = split(i)
        return remote(
            fields_ref.at[q, part], halo.at[slot, q, part], send_p, recv_p.at[lax.rem(i, ring)], place(partner)
        )

    def relay(i, slot):
        q, part = split(i)
        return remote(
            halo.at[1 - side, q, part],
            halo.at[slot, q, part],
            send_r.at[(q >= planes_all - NEAR).astype(jnp.int32)],
            recv_r.at[q // depth],
            place(follow),
        )

    def detour(planes):
        picked = pl.ds(planes_all - planes, planes)
        return remote(
            fields_ref.at[picked], passing.at[pl.ds(NEAR - planes, planes)], send_d, recv_d, place(other)
        )

    def hand_on(k):
        q = planes_all - k
        return remote(
            passing.at[NEAR - k], halo.at[1 - side, q], send_h.at[k - 1], recv_r.at[q // depth], place(partner)
        )

    def spread(target, source):
        return remote(wloc.at[target], wrecv.at[source], send_w, recv_w, (grp, target))

    pl.semaphore_wait(barrier, jnp.where(first, 2, 3))

    @pl.loop(0, ahead)
    def _(i):
        exchange(i, side).start()

    @pl.when(jnp.logical_not(first))
    def _():
        detour(NEAR).start()

    @pl.when(jnp.logical_not(first))
    def _():
        @pl.when(jnp.logical_not(second))
        def _():
            pl.semaphore_wait(chain_sem, 1)

        @pl.when(last)
        def _():
            signal(wrap_sem, (behind_grp, dev))

        @pl.when(jnp.logical_not(last))
        def _():
            signal(chain_sem, (grp, dev + step))

    load.start()
    for copy in small:
        copy.start()

    rhs_ref[...] = jnp.zeros_like(rhs_ref)
    load.wait()
    for copy in small:
        copy.wait()
    for c in range(count):
        for k in range(TAIL):
            coef_ref[c, k] = jnp.full((8, width), mix_ref[c, count - TAIL + k], jnp.float32)
            coef_ref[c, TAIL + k] = jnp.full((8, width), lap_ref[c, count - TAIL + k], jnp.float32)
    for k in range(TAIL):
        for p in range(depth):
            tail_ref[k, p] = own[(count - TAIL + k) * depth + p]

    @pl.when(last)
    def _():
        pl.semaphore_wait(wrap_sem, 1)

    def advance(i):
        exchange(i, 1 - side).wait_recv()
        q, _ = split(i)

        @pl.when((q < planes_all - NEAR) | (last & (q < planes_all - FAR)))
        def _():
            relay(i, side).start()

        @pl.when(i + ahead < chunks)
        def _():
            exchange(i + ahead, side).start()

    @pl.loop(0, LAG * depth * HALVES)
    def _(i):
        advance(i)

    def relayed(g):
        part = pl.ds(g * depth, depth)
        remote(halo.at[side, part], halo.at[side, part], send_r.at[0], recv_r.at[g], place(follow)).wait_recv()

    def weyl_local(part):
        tiles = rows // 8
        share = depth * tiles // WEYL_STEPS

        @pl.loop(0, share)
        def _(u):
            t = part * share + u
            p = t // tiles
            start = pl.multiple_of(lax.rem(t, tiles) * 8, 8)
            strip = pl.ds(start, 8)
            curv = [own[(6 + n) * depth + p, strip, :] for n in range(6)]
            lap = [laph[n, p, strip, :] for n in range(6)]
            grad = [[gradk[n, a, p, strip, :] for n in range(6)] for a in range(3)]
            lane = lax.broadcasted_iota(jnp.int32, (8, width), 1)
            row = lax.broadcasted_iota(jnp.int32, (8, width), 0) + start
            layer = jnp.full((8, width), slab * depth + p, jnp.int32)
            along_x = lane.astype(jnp.float32) + (0.5 - 0.5 * width)
            along_y = row.astype(jnp.float32) + (0.5 - 0.5 * rows)
            along_z = layer.astype(jnp.float32) + (0.5 - 0.5 * depth * slabs)
            real, imag = weyl_pair(curv, lap, grad, along_x, along_y, along_z)
            wtmp[0, p, strip, :] = real
            wtmp[1, p, strip, :] = imag

    def stencil(f, planes, p):
        zm2, zm1, _, zp1, zp2 = planes[p : p + 5]
        ym1, ym2 = pltpu.roll(f, 1, 0), pltpu.roll(f, 2, 0)
        yp1, yp2 = pltpu.roll(f, rows - 1, 0), pltpu.roll(f, rows - 2, 0)
        xm1, xm2 = pltpu.roll(f, 1, 1), pltpu.roll(f, 2, 1)
        xp1, xp2 = pltpu.roll(f, width - 1, 1), pltpu.roll(f, width - 2, 1)
        near = ((zm1 + zp1) + (ym1 + yp1)) + (xm1 + xp1)
        far_sum = ((zm2 + zp2) + (ym2 + yp2)) + (xm2 + xp2)
        lap = (16.0 * near - far_sum - 90.0 * f) * (1.0 / 12.0)
        gz = (8.0 * (zp1 - zm1) - (zp2 - zm2)) * (1.0 / 12.0)
        gy = (8.0 * (yp1 - ym1) - (yp2 - ym2)) * (1.0 / 12.0)
        gx = (8.0 * (xp1 - xm1) - (xp2 - xm2)) * (1.0 / 12.0)
        return lap, gx, gy, gz

    def process(g, p):
        q = g * depth
        planes = [halo[0, q], halo[0, q + 1], own[q], own[q + 1], halo[1, q], halo[1, q + 1]]
        lap, gx, gy, gz = stencil(own[q + p], planes, p)
        lapbuf[p] = lap
        rhs_ref[g, p] += own[12 * depth + p] * gz + own[13 * depth + p] * gy + own[14 * depth + p] * gx

        @pl.when(g < 6)
        def _():
            laph[g, p] = lap

        @pl.when(jnp.logical_and(g >= 6, g < 12))
        def _():
            gradk[g - 6, 0, p] = gx
            gradk[g - 6, 1, p] = gy
            gradk[g - 6, 2, p] = gz

        @pl.loop(0, rows // MIX)
        def _(t):
            strip = pl.ds(pl.multiple_of(t * MIX, MIX), MIX)
            f = own[q + p, strip, :]
            lap = lapbuf[p, strip, :]
            for c in range(count):
                rhs_ref[c, p, strip, :] += mix_ref[c, g] * f + lap_ref[c, g] * lap

    def without_far(g, p):
        q = g * depth
        zero = jnp.zeros(own.shape[1:], jnp.float32)
        for parity in range(2):

            @pl.when(side == parity)
            def _():
                low = [zero] * depth if parity == 0 else [halo[0, q + k] for k in range(depth)]
                high = [zero] * depth if parity == 1 else [halo[1, q + k] for k in range(depth)]
                planes = low + [own[q + k] for k in range(depth)] + high
                lap, gx, gy, gz = stencil(own[q + p], planes, p)
                tail_ref[g - (count - 2 * TAIL), p] = lap
                rhs_ref[g, p] += (
                    own[12 * depth + p] * gz + own[13 * depth + p] * gy + own[14 * depth + p] * gx
                )

    def far_share(g, p):
        q = g * depth
        for parity in range(2):

            @pl.when(side == parity)
            def _():
                away = depth - 1 - p if parity == 1 else p
                sign = 1.0 if parity == 1 else -1.0
                near, beyond = (q, q + 1) if parity == 1 else (q + 1, q)
                if away == 0:
                    one, two = halo[parity, near], halo[parity, beyond]
                    lap = (16.0 * one - two) * (1.0 / 12.0)
                    gz = (8.0 * one - two) * (sign / 12.0)
                else:
                    two = halo[parity, near]
                    lap = two * (-1.0 / 12.0)
                    gz = two * (-sign / 12.0)
                tail_ref[g - (count - 2 * TAIL), p] += lap
                rhs_ref[g, p] += own[12 * depth + p] * gz

    @pl.loop(0, count - TAIL)
    def _(g):
        more = g + LAG < count

        @pl.when(more)
        def _():
            for k in range(HALVES):
                advance((g + LAG) * depth * HALVES + k)

        relayed(g)
        process(g, 0)

        @pl.when(more)
        def _():
            for k in range(HALVES):
                advance((g + LAG) * depth * HALVES + HALVES + k)

        process(g, 1)

        @pl.when((g == LEAVE) & first)
        def _():
            detour(FAR).start()

        @pl.when((g == PASS) & last)
        def _():
            detour(FAR).wait_recv()
            for k in range(FAR, 0, -1):
                hand_on(k).start()

        @pl.when((g == PASS) & jnp.logical_not(last))
        def _():
            detour(NEAR).wait_recv()
            for k in range(NEAR, 0, -1):
                hand_on(k).start()

        @pl.when(jnp.logical_and(g >= 11, g < 11 + WEYL_STEPS))
        def _():
            weyl_local(g - 11)

        @pl.when(g == 11 + WEYL_STEPS)
        def _():
            for m in range(members):
                wloc[m] = wtmp[:, :, m * per : (m + 1) * per, :]
            wrecv[dev] = wloc[dev]

        @pl.when(g == jnp.where(lax.rem(grp, 2) == 0, SPREAD_EVEN, SPREAD_ODD))
        def _():
            for offset in range(1, members):
                spread(peer(offset), dev).start()

    for g in range(count - TAIL, count):
        for p in range(depth):
            without_far(g, p)
    for g in range(count - 1, count - TAIL - 1, -1):
        relayed(g)
        for p in range(depth):
            far_share(g, p)

    others = pl.ds(0, members - 1)
    remote(wrecv.at[others], wrecv.at[others], send_w, recv_w, (grp, dev)).wait_recv()
    remote(wloc.at[others], wloc.at[others], send_w, recv_w, (grp, dev)).wait_send()
    remote(own, halo.at[0], send_p, recv_p.at[0], place(partner)).wait_send()
    def totals(planes, semaphore):
        part = pl.ds(0, planes)
        remote(halo.at[0, part], halo.at[0, part], semaphore, recv_r.at[0], place(follow)).wait_send()

    totals(planes_all - NEAR, send_r.at[0])

    @pl.when(last)
    def _():
        totals(NEAR - FAR, send_r.at[1])

    for k in range(NEAR, 0, -1):
        if k <= FAR:
            hand_on(k).wait_send()
        else:

            @pl.when(jnp.logical_not(last))
            def _():
                hand_on(k).wait_send()

    @pl.when(first)
    def _():
        detour(FAR).wait_send()

    @pl.when(jnp.logical_not(first))
    def _():
        detour(NEAR).wait_send()


def finish(members, part_ref, wrecv, tail_ref, coef_ref, rhs_ref, weyl_ref, whole, rhs_sem, weyl_sem):
    count, depth, rows, width = part_ref.shape
    blocks = []
    for source in range(members):
        layers = pl.ds(source * depth, depth)
        blocks.append(
            pltpu.make_async_copy(wrecv.at[source], weyl_ref.at[:, layers], weyl_sem)
        )
    for block in blocks:
        block.start()

    @pl.loop(0, depth * (rows // STRIP))
    def _(t):
        p = t // (rows // STRIP)
        start = pl.multiple_of(lax.rem(t, rows // STRIP) * STRIP, STRIP)
        strip = pl.ds(start, STRIP)
        terms = [
            [tail_ref[k, p, pl.ds(start + 8 * r, 8), :] for r in range(STRIP // 8)] for k in range(2 * TAIL)
        ]
        for c in range(count):
            coefs = [coef_ref[c, k] for k in range(2 * TAIL)]
            for r in range(STRIP // 8):
                part = pl.ds(start + 8 * r, 8)
                value = part_ref[c, p, part, :]
                for k in range(2 * TAIL):
                    value = value + coefs[k] * terms[k][r]
                whole[c, p, part, :] = value
        pltpu.make_async_copy(whole.at[:, p, strip], rhs_ref.at[:, p, strip], rhs_sem).start()

    pltpu.make_async_copy(weyl_ref, weyl_ref, weyl_sem).wait()
    pltpu.make_async_copy(whole, rhs_ref, rhs_sem).wait()


def per_device(groups, members, fields, mix_matrix, laplace_matrix):
    count, depth, rows, width = fields.shape
    assert depth == 2 and members % 4 == 0
    plane = (rows, width)
    per = rows // members
    vmem = functools.partial(pltpu.VMEM, dtype=jnp.float32)
    dma = pltpu.SemaphoreType.DMA
    in_hbm, in_vmem = pl.BlockSpec(memory_space=pltpu.HBM), pl.BlockSpec(memory_space=pltpu.VMEM)
    share = functools.partial(jax.ShapeDtypeStruct, dtype=jnp.float32)
    pieces = pl.pallas_call(
        functools.partial(kernel, groups, members),
        out_shape=(
            share(fields.shape),
            share((members, 2, depth, per, width)),
            share((2 * TAIL, depth) + plane),
            share((count, 2 * TAIL, 8, width)),
        ),
        in_specs=[in_hbm] * 3,
        out_specs=(in_vmem,) * 4,
        scratch_shapes=[
            vmem((count * depth,) + plane),
            vmem((2, count * depth) + plane),
            vmem((depth,) + plane),
            vmem((6, depth) + plane),
            vmem((6, 3, depth) + plane),
            vmem((2, depth) + plane),
            vmem((members, 2, depth, per, width)),
            vmem((NEAR,) + plane),
            pltpu.SMEM((count, count), jnp.float32),
            pltpu.SMEM((count, count), jnp.float32),
            dma,
            dma((2,)),
            dma,
            dma((2 * min(AHEAD, count * depth * HALVES),)),
            dma((2,)),
            dma((count,)),
            dma,
            dma,
            dma((NEAR,)),
            dma,
            dma,
            pltpu.SemaphoreType.REGULAR,
            pltpu.SemaphoreType.REGULAR,
        ],
        compiler_params=pltpu.CompilerParams(
            collective_id=0, has_side_effects=True, vmem_limit_bytes=32 * 1024 * 1024
        ),
        name="evolve",
    )(
        pltpu.with_memory_space_constraint(fields.reshape((count * depth,) + plane), pltpu.HBM),
        pltpu.with_memory_space_constraint(mix_matrix, pltpu.HBM),
        pltpu.with_memory_space_constraint(laplace_matrix, pltpu.HBM),
    )
    return pl.pallas_call(
        functools.partial(finish, members),
        out_shape=(share(fields.shape), share((2, depth * members, per, width))),
        in_specs=[in_vmem] * 4,
        out_specs=(in_hbm,) * 2,
        scratch_shapes=[vmem((count, depth) + plane), dma, dma],
        compiler_params=pltpu.CompilerParams(vmem_limit_bytes=8 * 1024 * 1024),
        name="finish",
    )(*pieces)


def solution(mesh):
    groups, members = mesh.shape["grp"], mesh.shape["dev"]
    return jax.shard_map(
        functools.partial(per_device, groups, members),
        mesh=mesh,
        in_specs=(P(None, ("grp", "dev"), None, None), P(), P()),
        out_specs=(P(None, ("grp", "dev"), None, None), P(None, "grp", "dev", None)),
        check_vma=False,
    )
```
